32 devices in a mesh: dp: 8 (over z, core), row: 2 (over x), col: 2 (over y).
Axes of the slice: x: 2, y: 2, z: 4, core: 2. Of those that a mesh axis runs over, the one named last changes fastest.
Arguments:
- tokens: bfloat16 [4096, 8192], P(('dp', 'row', 'col')), parts along dimension 0, may hold values from -6 to 6
- w_gate: bfloat16 [8192, 1024], P(('row', 'col')), may hold values from -0.0625 to 0.0625
- w_up: bfloat16 [8192, 1024], P(('row', 'col')), may hold values from -0.0625 to 0.0625
- w_down: bfloat16 [1024, 8192], P(None, ('row', 'col')), may hold values from -0.1875 to 0.1875
Outputs:
- mixed: bfloat16 [4096, 8192], P(('dp', 'row', 'col')), parts along dimension 0
The draws below stay inside these ranges and needn't reach their ends.
There are 8 independent parts, one for each index of `dp`. The reference program is written for one: setup_inputs(seed, part) draws one part's arguments, and reference() takes and returns one part's arrays. A program takes and returns all parts, laid end to end along the dimension named above; an argument that names none is the same for every part. Nothing has to cross between parts.
All inputs are finite; a program needn't handle non-finite values.
Results may differ from the reference program's by a relative error of at most 0.029.
Values may be sent and summed in bfloat16 or wider, within the bound.
No kernel may reach another device: no remote copies, remote signals or barrier semaphores. Data moves between devices by JAX's collectives and lax.ppermute only.
A program may use at most 64 MiB of HBM per device.

```python
import jax
import jax.numpy as jnp
from jax import lax

D = 8192
H = 1024
TOKENS = 512
N_ROW = 2


def block_scale(rng, shape, pieces, low, largest):
    loudness = 1.0
    for axis_at, shards_of in pieces:
        draws = jax.random.uniform(jax.random.fold_in(jax.random.fold_in(rng, 6), axis_at), (shards_of,), jnp.float32, low / len(pieces), largest / len(pieces))
        loudness = loudness * jnp.repeat(jnp.exp(draws), shape[axis_at] // shards_of).reshape((-1,) + (1,) * (len(shape) - 1 - axis_at))
    return loudness


def noise(own_key, shape, width, bound, shards=(), dtype=jnp.bfloat16):
    level = block_scale(own_key, shape, shards, -0.22, 0.18) if shards else 1.0
    entries = jax.random.normal(own_key, shape, jnp.float32) * width * level
    return jnp.minimum(jnp.maximum(entries, -bound), bound).astype(dtype)


def setup_inputs(seed: int = 0, part: int = 0) -> dict:
    seeds = jax.random.split(jax.random.key(seed), 5)
    part_splits = jax.random.split(jax.random.fold_in(seeds[4], part), 5)
    return {
        "tokens": noise(part_splits[0], (TOKENS, D), 1.0, 6.0, ((0, 4),)),
        "w_gate": noise(seeds[1], (D, H), D ** -0.5, 0.0625, ((0, 4),)),
        "w_up": noise(seeds[2], (D, H), D ** -0.5, 0.0625, ((0, 4),)),
        "w_down": noise(seeds[3], (H, D), H ** -0.5, 0.1875, ((1, 4),)),
    }


def reference(tokens, w_gate, w_up, w_down):
    slab_width = D // N_ROW
    paired = jnp.concatenate([w_gate, w_up], axis=1)
    running = jnp.zeros((tokens.shape[0], 2 * H), jnp.float32)
    for block_index in range(N_ROW):
        lower = block_index * slab_width
        upper = lower + slab_width
        partial_value = jnp.dot(tokens[:, lower:upper], paired[lower:upper], preferred_element_type=jnp.float32)
        rounded = lax.optimization_barrier(partial_value.astype(jnp.bfloat16))
        running = running + rounded.astype(jnp.float32)
    hidden = (jax.nn.silu(running[:, :H]) * running[:, H:]).astype(jnp.bfloat16)
    return jnp.dot(hidden, w_down, preferred_element_type=jnp.float32).astype(jnp.bfloat16)
```

```python
import jax
import jax.numpy as jnp
from jax import lax
from jax.sharding import PartitionSpec as P


def solution(mesh):
    rows, cols = mesh.shape["row"], mesh.shape["col"]
    shifts = [(dr, dc) for dr in range(rows) for dc in range(cols)]
    away = [s for s in shifts if s != (0, 0)]

    def send(x, shift):
        dr, dc = shift
        pairs = [
            (r * cols + c, (r + dr) % rows * cols + (c + dc) % cols) for r in range(rows) for c in range(cols)
        ]
        return lax.ppermute(x, ("row", "col"), pairs)

    def shards(tokens, w_gate, w_up, w_down):
        r, c = lax.axis_index("row"), lax.axis_index("col")
        slab = w_gate.shape[0]
        width = w_down.shape[1]

        def place(shift):
            return (r + shift[0]) % rows * cols + (c + shift[1]) % cols

        def back(shift):
            return (-shift[0]) % rows, (-shift[1]) % cols

        feats = {s: lax.dynamic_slice_in_dim(tokens, place(s) * slab, slab, axis=1) for s in shifts}
        got = {s: send(feats[s], s) for s in away}
        got[0, 0] = feats[0, 0]
        parts = {}
        for s in away + [(0, 0)]:
            gate = jnp.dot(got[s], w_gate, preferred_element_type=jnp.float32)
            up = jnp.dot(got[s], w_up, preferred_element_type=jnp.float32)
            parts[s] = (gate.astype(jnp.bfloat16), up.astype(jnp.bfloat16)) if s != (0, 0) else (gate, up)
        gate, up = parts[0, 0]
        home = {s: tuple(send(p, back(s)) for p in parts[s]) for s in away}
        for s in away:
            gate = gate + home[s][0].astype(jnp.float32)
            up = up + home[s][1].astype(jnp.float32)
        hidden = (jax.nn.silu(gate) * up).astype(jnp.bfloat16)
        others = {s: send(hidden, s) for s in away}
        others[0, 0] = hidden
        outs = {}
        for s in away + [(0, 0)]:
            out = jnp.dot(others[s], w_down, preferred_element_type=jnp.float32).astype(jnp.bfloat16)
            outs[s] = send(out, back(s)) if s != (0, 0) else out
        mixed = jnp.zeros((tokens.shape[0], width * rows * cols), jnp.bfloat16)
        for s in shifts:
            mixed = lax.dynamic_update_slice_in_dim(mixed, outs[s], place(s) * width, axis=1)
        return mixed

    in_specs = (
        P(("dp", "row", "col"), None),
        P(("row", "col"), None),
        P(("row", "col"), None),
        P(None, ("row", "col")),
    )
    out_specs = P(("dp", "row", "col"), None)
    return jax.shard_map(shards, mesh=mesh, in_specs=in_specs, out_specs=out_specs, check_vma=False)
```

```python
import jax
import jax.numpy as jnp
from jax import lax
from jax.sharding import PartitionSpec as P


def solution(mesh):
    rows, cols = mesh.shape["row"], mesh.shape["col"]
    shifts = [(dr, dc) for dr in range(rows) for dc in range(cols)]
    away = [s for s in shifts if s != (0, 0)]

    def send(x, shift):
        dr, dc = shift
        pairs = [
            (r * cols + c, (r + dr) % rows * cols + (c + dc) % cols) for r in range(rows) for c in range(cols)
        ]
        return lax.ppermute(x, ("row", "col"), pairs)

    def shards(tokens, w_gate, w_up, w_down):
        r, c = lax.axis_index("row"), lax.axis_index("col")
        slab = w_gate.shape[0]
        width = w_down.shape[1]

        def place(shift):
            return (r + shift[0]) % rows * cols + (c + shift[1]) % cols

        def back(shift):
            return (-shift[0]) % rows, (-shift[1]) % cols

        feats = {s: lax.dynamic_slice_in_dim(tokens, place(s) * slab, slab, axis=1) for s in shifts}
        got = {s: send(feats[s], s) for s in away}
        got[0, 0] = feats[0, 0]
        order = away + [(0, 0)]

        def reduced(weight, col_first):
            first, second = (cols, rows) if col_first else (rows, cols)

            def shift(a, b):
                return (b, a) if col_first else (a, b)

            parts = {s: jnp.dot(got[s], weight, preferred_element_type=jnp.float32) for s in order}
            sums = {b: parts[shift(0, b)] for b in range(second)}
            for b in reversed(range(second)):
                for a in range(1, first):
                    part = send(parts[shift(a, b)].astype(jnp.bfloat16), back(shift(a, 0)))
                    sums[b] = sums[b] + part.astype(jnp.float32)
            total = sums[0]
            for b in range(1, second):
                total = total + send(sums[b].astype(jnp.bfloat16), back(shift(0, b))).astype(jnp.float32)
            return total

        gate, up = reduced(w_gate, True), reduced(w_up, False)
        hidden = (jax.nn.silu(gate) * up).astype(jnp.bfloat16)
        others = {s: send(hidden, s) for s in away}
        others[0, 0] = hidden
        outs = {}
        for s in away + [(0, 0)]:
            out = jnp.dot(others[s], w_down, preferred_element_type=jnp.float32).astype(jnp.bfloat16)
            outs[s] = send(out, back(s)) if s != (0, 0) else out
        mixed = jnp.zeros((tokens.shape[0], width * rows * cols), jnp.bfloat16)
        for s in shifts:
            mixed = lax.dynamic_update_slice_in_dim(mixed, outs[s], place(s) * width, axis=1)
        return mixed

    in_specs = (
        P(("dp", "row", "col"), None),
        P(("row", "col"), None),
        P(("row", "col"), None),
        P(None, ("row", "col")),
    )
    out_specs = P(("dp", "row", "col"), None)
    return jax.shard_map(shards, mesh=mesh, in_specs=in_specs, out_specs=out_specs, check_vma=False)
```

```python
import jax
import jax.numpy as jnp
from jax import lax
from jax.sharding import PartitionSpec as P


def solution(mesh):
    rows, cols, dp = mesh.shape["row"], mesh.shape["col"], mesh.shape["dp"]
    cores = 2 if dp % 2 == 0 else 1
    chips = dp // cores
    shifts = [(dr, dc) for dr in range(rows) for dc in range(cols)]
    away = [s for s in shifts if s != (0, 0)]

    def send(x, shift):
        dr, dc = shift
        pairs = [
            (r * cols + c, (r + dr) % rows * cols + (c + dc) % cols) for r in range(rows) for c in range(cols)
        ]
        return lax.ppermute(x, ("row", "col"), pairs)

    def send_dp(x, chip_shift, core_shift):
        pairs = [
            (z * cores + k, (z + chip_shift) % chips * cores + (k + core_shift) % cores)
            for z in range(chips)
            for k in range(cores)
        ]
        return lax.ppermute(x, "dp", pairs)

    def back(shift):
        return (-shift[0]) % rows, (-shift[1]) % cols

    def matmul(a, b):
        return jnp.dot(a, b, preferred_element_type=jnp.float32)

    def shards(tokens, w_gate, w_up, w_down):
        r, c, d = lax.axis_index("row"), lax.axis_index("col"), lax.axis_index("dp")
        chip, core = d // cores, d % cores
        slab = w_gate.shape[0]
        hidden_width, width = w_down.shape
        half = width // 2
        share = hidden_width // dp

        def place(shift):
            return (r + shift[0]) % rows * cols + (c + shift[1]) % cols

        piece = lax.dynamic_slice_in_dim(w_down, d * share, share, axis=0)
        held = jnp.concatenate(
            [send(piece[:, :half], back((0, dc))) for dc in range(1, cols)]
            + [send(piece[:, half:], back((dr, 0))) for dr in range(1, rows)],
            axis=1,
        )

        feats = {s: lax.dynamic_slice_in_dim(tokens, place(s) * slab, slab, axis=1) for s in shifts}
        got = {s: send(feats[s], s) for s in away}
        got[0, 0] = feats[0, 0]

        far = jnp.zeros((hidden_width, held.shape[1]), jnp.bfloat16)
        for z in range(chips):
            from_chip = send_dp(held, z, 0) if z else held
            for k in range(cores):
                rows_held = send_dp(from_chip, 0, k) if k else from_chip
                at = ((chip - z) % chips * cores + (core - k) % cores) * share
                far = lax.dynamic_update_slice_in_dim(far, rows_held, at, axis=0)

        def reduced(weight, col_first):
            first, second = (cols, rows) if col_first else (rows, cols)

            def shift(a, b):
                return (b, a) if col_first else (a, b)

            parts = {s: matmul(got[s], weight) for s in shifts}
            sums = {b: parts[shift(0, b)] for b in range(second)}
            for b in reversed(range(second)):
                for a in range(1, first):
                    part = send(parts[shift(a, b)].astype(jnp.bfloat16), back(shift(a, 0)))
                    sums[b] = sums[b] + part.astype(jnp.float32)
            total = sums[0]
            for b in range(1, second):
                total = total + send(sums[b].astype(jnp.bfloat16), back(shift(0, b))).astype(jnp.float32)
            return total

        gate, up = reduced(w_gate, True), reduced(w_up, False)
        hidden = (jax.nn.silu(gate) * up).astype(jnp.bfloat16)

        split = half * (cols - 1)
        near = {(dr, 0): send(hidden, back((dr, 0))) for dr in range(1, rows)}
        near |= {(0, dc): send(hidden, back((0, dc))) for dc in range(1, cols)}
        landed = []
        own = matmul(hidden, w_down).astype(jnp.bfloat16)
        landed.append((own, place((0, 0)) * width))
        for s, other in near.items():
            weight = w_down[:, :half] if s[1] == 0 else w_down[:, half:]
            out = send(matmul(other, weight).astype(jnp.bfloat16), s)
            landed.append((out, place(back(s)) * width + (0 if s[1] == 0 else half)))
        for s, other in near.items():
            weight = far[:, :split] if s[1] == 0 else far[:, split:]
            out = send(matmul(other, weight).astype(jnp.bfloat16), s)
            for i in range(1, cols if s[1] == 0 else rows):
                turn = (-s[0], i) if s[1] == 0 else (i, -s[1])
                landed.append(
                    (out[:, (i - 1) * half : i * half], place(turn) * width + (0 if s[1] == 0 else half))
                )
        own_far = matmul(hidden, far).astype(jnp.bfloat16)
        for dc in range(1, cols):
            landed.append((own_far[:, (dc - 1) * half : dc * half], place((0, dc)) * width))
        for dr in range(1, rows):
            lower = split + (dr - 1) * half
            landed.append((own_far[:, lower : lower + half], place((dr, 0)) * width + half))

        mixed = jnp.zeros((tokens.shape[0], width * rows * cols), jnp.bfloat16)
        for block, at in landed:
            mixed = lax.dynamic_update_slice_in_dim(mixed, block, at, axis=1)
        return mixed

    in_specs = (
        P(("dp", "row", "col"), None),
        P(("row", "col"), None),
        P(("row", "col"), None),
        P(None, ("row", "col")),
    )
    out_specs = P(("dp", "row", "col"), None)
    return jax.shard_map(shards, mesh=mesh, in_specs=in_specs, out_specs=out_specs, check_vma=False)
```

```python
import jax
import jax.numpy as jnp
from jax import lax
from jax.sharding import PartitionSpec as P


def solution(mesh):
    rows, cols, dp = mesh.shape["row"], mesh.shape["col"], mesh.shape["dp"]
    cores = 2 if dp % 2 == 0 else 1
    chips = dp // cores
    shifts = [(dr, dc) for dr in range(rows) for dc in range(cols)]
    away = [s for s in shifts if s != (0, 0)]

    def send(x, shift):
        dr, dc = shift
        pairs = [
            (r * cols + c, (r + dr) % rows * cols + (c + dc) % cols) for r in range(rows) for c in range(cols)
        ]
        return lax.ppermute(x, ("row", "col"), pairs)

    def send_dp(x, chip_shift, core_shift):
        pairs = [
            (z * cores + k, (z + chip_shift) % chips * cores + (k + core_shift) % cores)
            for z in range(chips)
            for k in range(cores)
        ]
        return lax.ppermute(x, "dp", pairs)

    def back(shift):
        return (-shift[0]) % rows, (-shift[1]) % cols

    def matmul(a, b):
        return jnp.dot(a, b, preferred_element_type=jnp.float32)

    def shards(tokens, w_gate, w_up, w_down):
        r, c, d = lax.axis_index("row"), lax.axis_index("col"), lax.axis_index("dp")
        chip, core = d // cores, d % cores
        slab = w_gate.shape[0]
        hidden_width, width = w_down.shape
        half = width // 2
        share = hidden_width // dp

        def place(shift):
            return (r + shift[0]) % rows * cols + (c + shift[1]) % cols

        piece = lax.dynamic_slice_in_dim(w_down, d * share, share, axis=0)
        held = jnp.concatenate(
            [send(piece[:, :half], back((0, dc))) for dc in range(1, cols)]
            + [send(piece[:, half:], back((dr, 0))) for dr in range(1, rows)],
            axis=1,
        )

        feats = {s: lax.dynamic_slice_in_dim(tokens, place(s) * slab, slab, axis=1) for s in shifts}
        got = {s: send(feats[s], s) for s in away}
        got[0, 0] = feats[0, 0]

        from_chips = [send_dp(held, z, 0) if z else held for z in range(chips)]

        def reduced(weight, col_first):
            first, second = (cols, rows) if col_first else (rows, cols)

            def shift(a, b):
                return (b, a) if col_first else (a, b)

            parts = {s: matmul(got[s], weight) for s in away}
            parts[0, 0] = matmul(got[0, 0], weight)
            sums = {b: parts[shift(0, b)] for b in range(second)}
            for b in reversed(range(second)):
                for a in range(1, first):
                    part = send(parts[shift(a, b)].astype(jnp.bfloat16), back(shift(a, 0)))
                    sums[b] = sums[b] + part.astype(jnp.float32)
            total = sums[0]
            for b in range(1, second):
                total = total + send(sums[b].astype(jnp.bfloat16), back(shift(0, b))).astype(jnp.float32)
            return total

        gate, up = reduced(w_gate, True), reduced(w_up, False)
        hidden = (jax.nn.silu(gate) * up).astype(jnp.bfloat16)

        split = half * (cols - 1)
        near = {(dr, 0): send(hidden, back((dr, 0))) for dr in range(1, rows)}
        near |= {(0, dc): send(hidden, back((0, dc))) for dc in range(1, cols)}
        far = jnp.zeros((hidden_width, held.shape[1]), jnp.bfloat16)
        for z in range(chips):
            from_chip, _ = lax.optimization_barrier((from_chips[z], hidden)) if z else (held, None)
            for k in range(cores):
                rows_held = send_dp(from_chip, 0, k) if k else from_chip
                at = ((chip - z) % chips * cores + (core - k) % cores) * share
                far = lax.dynamic_update_slice_in_dim(far, rows_held, at, axis=0)

        landed = []
        own = matmul(hidden, w_down).astype(jnp.bfloat16)
        landed.append((own, place((0, 0)) * width))
        own_far = matmul(hidden, far).astype(jnp.bfloat16)
        for dc in range(1, cols):
            landed.append((own_far[:, (dc - 1) * half : dc * half], place((0, dc)) * width))
        for dr in range(1, rows):
            lower = split + (dr - 1) * half
            landed.append((own_far[:, lower : lower + half], place((dr, 0)) * width + half))
        for s, other in near.items():
            weight = w_down[:, :half] if s[1] == 0 else w_down[:, half:]
            out = send(matmul(other, weight).astype(jnp.bfloat16), s)
            landed.append((out, place(back(s)) * width + (0 if s[1] == 0 else half)))
        for s, other in near.items():
            weight = far[:, :split] if s[1] == 0 else far[:, split:]
            out = send(matmul(other, weight).astype(jnp.bfloat16), s)
            for i in range(1, cols if s[1] == 0 else rows):
                turn = (-s[0], i) if s[1] == 0 else (i, -s[1])
                landed.append(
                    (out[:, (i - 1) * half : i * half], place(turn) * width + (0 if s[1] == 0 else half))
                )
        mixed = jnp.zeros((tokens.shape[0], width * rows * cols), jnp.bfloat16)
        for block, at in landed:
            mixed = lax.dynamic_update_slice_in_dim(mixed, block, at, axis=1)
        return mixed

    in_specs = (
        P(("dp", "row", "col"), None),
        P(("row", "col"), None),
        P(("row", "col"), None),
        P(None, ("row", "col")),
    )
    out_specs = P(("dp", "row", "col"), None)
    return jax.shard_map(shards, mesh=mesh, in_specs=in_specs, out_specs=out_specs, check_vma=False)
```

```python
import jax
import jax.numpy as jnp
from jax import lax
from jax.sharding import PartitionSpec as P


def solution(mesh):
    rows, cols, dp = mesh.shape["row"], mesh.shape["col"], mesh.shape["dp"]
    cores = 2 if dp % 2 == 0 else 1
    chips = dp // cores
    shifts = [(dr, dc) for dr in range(rows) for dc in range(cols)]
    away = [s for s in shifts if s != (0, 0)]

    def send(x, shift):
        dr, dc = shift
        pairs = [
            (r * cols + c, (r + dr) % rows * cols + (c + dc) % cols) for r in range(rows) for c in range(cols)
        ]
        return lax.ppermute(x, ("row", "col"), pairs)

    def send_dp(x, chip_pairs, core_shift):
        pairs = [(z * cores + k, to * cores + (k + core_shift) % cores) for z, to in chip_pairs for k in range(cores)]
        return lax.ppermute(x, "dp", pairs)

    def swap(x, core_shift):
        return send_dp(x, [(z, z) for z in range(chips)], core_shift)

    def back(shift):
        return (-shift[0]) % rows, (-shift[1]) % cols

    def matmul(a, b):
        return jnp.dot(a, b, preferred_element_type=jnp.float32)

    def shards(tokens, w_gate, w_up, w_down):
        r, c, d = lax.axis_index("row"), lax.axis_index("col"), lax.axis_index("dp")
        chip, core = d // cores, d % cores
        slab = w_gate.shape[0]
        hidden_width, width = w_down.shape
        half = width // 2
        share = hidden_width // dp

        def place(shift):
            return (r + shift[0]) % rows * cols + (c + shift[1]) % cols

        piece = lax.dynamic_slice_in_dim(w_down, d * share, share, axis=0)
        sides = [(0, dc) for dc in range(1, cols)] + [(dr, 0) for dr in range(1, rows)]
        held = jnp.concatenate([send(piece[:, half:] if s[0] else piece[:, :half], back(s)) for s in sides], axis=0)

        feats = {s: lax.dynamic_slice_in_dim(tokens, place(s) * slab, slab, axis=1) for s in shifts}
        got = {s: send(feats[s], s) for s in away}
        got[0, 0] = feats[0, 0]

        early, late = [], []
        if chips == 4:
            two = send_dp(held, [(z, z ^ 2) for z in range(chips)], 0)
            one = send_dp(held, [(z, z ^ 1) for z in range(chips)], 0)
            middle = send_dp(held, [(1, 2), (2, 1)], 0)
            early += [(one, chip ^ 1), (two, chip ^ 2)]
        else:
            for z in range(1, chips):
                turn = send_dp(held, [(i, (i + z) % chips) for i in range(chips)], 0)
                late.append((turn, (chip - z) % chips))

        def crossed(weight, col_first):
            first, second = (cols, rows) if col_first else (rows, cols)

            def shift(a, b):
                return (b, a) if col_first else (a, b)

            parts = {s: matmul(got[s], weight) for s in away}
            parts[0, 0] = matmul(got[0, 0], weight)
            sums = {b: parts[shift(0, b)] for b in range(second)}
            for b in reversed(range(second)):
                for a in range(1, first):
                    part = send(parts[shift(a, b)].astype(jnp.bfloat16), back(shift(a, 0)))
                    sums[b] = sums[b] + part.astype(jnp.float32)
            total = sums[0]
            passed = [sums[b].astype(jnp.bfloat16) for b in range(1, second)]
            for b in range(1, second):
                total = total + send(passed[b - 1], back(shift(0, b))).astype(jnp.float32)
            return total, passed

        gate, gate_passed = crossed(w_gate, True)
        up, up_passed = crossed(w_up, False)
        hidden = (jax.nn.silu(gate) * up).astype(jnp.bfloat16)

        if chips == 4:
            relayed = send_dp(two, [(2, 3), (1, 0)], 0)
            late.append((jnp.where((chip == 0) | (chip == chips - 1), relayed, middle), chip ^ 3))

        far = {s: jnp.zeros((hidden_width, half), jnp.bfloat16) for s in sides}

        def fill(pieces):
            for k in range(cores):
                for block, from_chip in pieces:
                    moved = swap(block, k) if k else block
                    at = (from_chip * cores + (core - k) % cores) * share
                    for i, s in enumerate(sides):
                        far[s] = lax.dynamic_update_slice_in_dim(far[s], moved[i * share : (i + 1) * share], at, axis=0)

        fill([(held, chip)])
        tied, _ = lax.optimization_barrier(([p for p, _ in early], gate_passed + up_passed))
        fill([(p, at) for p, (_, at) in zip(tied, early)])

        near = {s: send(hidden, back(s)) for s in reversed(sides)}
        landed = [(matmul(hidden, w_down).astype(jnp.bfloat16), place((0, 0)) * width)]
        outs = []
        for s, other in near.items():
            weight, at = (w_down[:, :half], 0) if s[1] == 0 else (w_down[:, half:], half)
            own_out = matmul(other, weight).astype(jnp.bfloat16)
            outs.append((send(own_out, s), place(back(s)) * width + at))

        tied, _ = lax.optimization_barrier(([p for p, _ in late], hidden))
        fill([(p, at) for p, (_, at) in zip(tied, late)])
        for s in sides:
            at = half if s[0] else 0
            landed.append((matmul(hidden, far[s]).astype(jnp.bfloat16), place(s) * width + at))
        for s, other in near.items():
            at = 0 if s[1] == 0 else half
            for t in sides:
                if (t[0] == 0) == (s[1] == 0):
                    far_out = send(matmul(other, far[t]).astype(jnp.bfloat16), s)
                    outs.append((far_out, place((t[0] - s[0], t[1] - s[1])) * width + at))
        landed += outs

        mixed = jnp.zeros((tokens.shape[0], width * rows * cols), jnp.bfloat16)
        for block, at in landed:
            mixed = lax.dynamic_update_slice_in_dim(mixed, block, at, axis=1)
        return mixed

    in_specs = (
        P(("dp", "row", "col"), None),
        P(("row", "col"), None),
        P(("row", "col"), None),
        P(None, ("row", "col")),
    )
    out_specs = P(("dp", "row", "col"), None)
    return jax.shard_map(shards, mesh=mesh, in_specs=in_specs, out_specs=out_specs, check_vma=False)
```

```python
import jax
import jax.numpy as jnp
from jax import lax
from jax.sharding import PartitionSpec as P


def solution(mesh):
    rows, cols, dp = mesh.shape["row"], mesh.shape["col"], mesh.shape["dp"]
    cores = 2 if dp % 2 == 0 else 1
    chips = dp // cores
    turned = cores == 2 and rows == cols
    line = turned and chips == 4
    count_a, count_b = cols, rows
    shifts = [(a, b) for a in range(count_a) for b in range(count_b)]
    away = [s for s in shifts if s != (0, 0)]

    def send(x, shift):
        pairs = []
        for d in range(dp):
            dr, dc = shift if turned and d % cores else shift[::-1]
            for r in range(rows):
                for c in range(cols):
                    to = (d * rows + (r + dr) % rows) * cols + (c + dc) % cols
                    pairs.append(((d * rows + r) * cols + c, to))
        return lax.ppermute(x, ("dp", "row", "col"), pairs)

    def send_dp(x, chip_pairs, core_shift):
        pairs = [(z * cores + k, to * cores + (k + core_shift) % cores) for z, to in chip_pairs for k in range(cores)]
        return lax.ppermute(x, "dp", pairs)

    def matmul(x, y):
        return jnp.dot(x, y, preferred_element_type=jnp.float32)

    def shards(tokens, w_gate, w_up, w_down):
        r, c, d = lax.axis_index("row"), lax.axis_index("col"), lax.axis_index("dp")
        chip, core = d // cores, d % cores
        slab = w_gate.shape[0]
        hidden_width, width = w_down.shape
        half = width // 2
        at_b = core * half if turned else 0
        at_a = half - at_b

        def place(a, b):
            dr, dc = (b + core * (a - b), a + core * (b - a)) if turned else (b, a)
            return (r + dr) % rows * cols + (c + dc) % cols

        def columns(x, at, size):
            return lax.dynamic_slice_in_dim(x, at, size, axis=1)

        early, late = [], []
        if turned:
            share = hidden_width // chips
            piece = lax.dynamic_slice(w_down, (chip * share, at_b), (share, half))
            held = [send(piece, (-a, 0)) for a in range(1, count_a)]
            held = held[0] if len(held) == 1 else jnp.concatenate(held, axis=0)

        feats = {s: columns(tokens, place(*s) * slab, slab) for s in shifts}
        got = {s: send(feats[s], s) for s in away}
        got[0, 0] = feats[0, 0]

        if line:
            two = send_dp(held, [(z, z ^ 2) for z in range(chips)], 0)
            one = send_dp(held, [(z, z ^ 1) for z in range(chips)], 0)
            middle = send_dp(held, [(1, 2), (2, 1)], 0)
            early += [(one, chip ^ 1), (two, chip ^ 2)]
        elif turned:
            for z in range(1, chips):
                turn = send_dp(held, [(i, (i + z) % chips) for i in range(chips)], 0)
                late.append((turn, (chip - z) % chips))

        def crossed(weight, a_first):
            first, second = (count_a, count_b) if a_first else (count_b, count_a)

            def shift(i, j):
                return (i, j) if a_first else (j, i)

            parts = {s: matmul(got[s], weight) for s in away}
            parts[0, 0] = matmul(got[0, 0], weight)
            sums = {j: parts[shift(0, j)] for j in range(second)}
            for j in reversed(range(second)):
                for i in range(1, first):
                    part = send(parts[shift(i, j)].astype(jnp.bfloat16), shift(-i, 0))
                    sums[j] = sums[j] + part.astype(jnp.float32)
            total = sums[0]
            passed = [sums[j].astype(jnp.bfloat16) for j in range(1, second)]
            for j in range(1, second):
                total = total + send(passed[j - 1], shift(0, -j)).astype(jnp.float32)
            return total, passed

        gate, gate_passed = crossed(w_gate, True)
        up, up_passed = crossed(w_up, False)
        hidden = (jax.nn.silu(gate) * up).astype(jnp.bfloat16)

        if turned:
            if line:
                relayed = send_dp(two, [(2, 3), (1, 0)], 0)
                late.append((jnp.where((chip == 0) | (chip == chips - 1), relayed, middle), chip ^ 3))
            far_b = {a: jnp.zeros((hidden_width, half), jnp.bfloat16) for a in range(1, count_a)}
            far_a = {b: jnp.zeros((hidden_width, half), jnp.bfloat16) for b in range(1, count_b)}

            def fill(far, block, from_chip):
                for i in far:
                    rows_of = block[(i - 1) * share : i * share]
                    far[i] = lax.dynamic_update_slice_in_dim(far[i], rows_of, from_chip * share, axis=0)

            def fill_both(pieces):
                for block, from_chip in pieces:
                    fill(far_b, block, from_chip)
                for block, from_chip in pieces:
                    fill(far_a, send_dp(block, [(z, z) for z in range(chips)], 1), from_chip)

            fill_both([(held, chip)])
            tied, _ = lax.optimization_barrier(([p for p, _ in early], gate_passed + up_passed))
            fill_both([(p, at) for p, (_, at) in zip(tied, early)])
        else:
            far_b = {a: send(w_down[:, :half], (-a, 0)) for a in range(1, count_a)}
            far_a = {b: send(w_down[:, half:], (0, -b)) for b in range(1, count_b)}

        near_b = {b: send(hidden, (0, -b)) for b in range(1, count_b)}
        near_a = {a: send(hidden, (-a, 0)) for a in range(1, count_a)}
        w_b, w_a = columns(w_down, at_b, half), columns(w_down, at_a, half)

        outs = []

        def give(x, weight, shift, slab_from, at):
            out = send(matmul(x, weight).astype(jnp.bfloat16), shift)
            outs.append((out, place(*slab_from) * width + at))

        for b, other in near_b.items():
            give(other, w_b, (0, b), (0, -b), at_b)
        for a, other in near_a.items():
            give(other, w_a, (a, 0), (-a, 0), at_a)
        if turned:
            tied, _ = lax.optimization_barrier(([p for p, _ in late], hidden))
            fill_both([(p, at) for p, (_, at) in zip(tied, late)])
        for b, other in near_b.items():
            for a in far_b:
                give(other, far_b[a], (0, b), (a, -b), at_b)
        for a, other in near_a.items():
            for b in far_a:
                give(other, far_a[b], (a, 0), (-a, b), at_a)

        landed = [(matmul(hidden, w_down).astype(jnp.bfloat16), place(0, 0) * width)]
        for a in far_b:
            landed.append((matmul(hidden, far_b[a]).astype(jnp.bfloat16), place(a, 0) * width + at_b))
        for b in far_a:
            landed.append((matmul(hidden, far_a[b]).astype(jnp.bfloat16), place(0, b) * width + at_a))
        mixed = jnp.zeros((tokens.shape[0], width * rows * cols), jnp.bfloat16)
        for block, at in landed + outs:
            mixed = lax.dynamic_update_slice_in_dim(mixed, block, at, axis=1)
        return mixed

    in_specs = (
        P(("dp", "row", "col"), None),
        P(("row", "col"), None),
        P(("row", "col"), None),
        P(None, ("row", "col")),
    )
    out_specs = P(("dp", "row", "col"), None)
    return jax.shard_map(shards, mesh=mesh, in_specs=in_specs, out_specs=out_specs, check_vma=False)
```

```python
import jax
import jax.numpy as jnp
from jax import lax
from jax.sharding import PartitionSpec as P


def solution(mesh):
    rows, cols, dp = mesh.shape["row"], mesh.shape["col"], mesh.shape["dp"]
    cores = 2 if dp % 2 == 0 else 1
    chips = dp // cores
    turned = cores == 2 and rows == cols
    line = turned and chips == 4
    shifts = [(dr, dc) for dr in range(rows) for dc in range(cols)]
    away = [s for s in shifts if s != (0, 0)]

    def send(x, shift):
        dr, dc = shift
        pairs = [
            (r * cols + c, (r + dr) % rows * cols + (c + dc) % cols) for r in range(rows) for c in range(cols)
        ]
        return lax.ppermute(x, ("row", "col"), pairs)

    def send_turned(x, shift):
        pairs = []
        for d in range(dp):
            dr, dc = shift if turned and d % cores else shift[::-1]
            for r in range(rows):
                for c in range(cols):
                    to = (d * rows + (r + dr) % rows) * cols + (c + dc) % cols
                    pairs.append(((d * rows + r) * cols + c, to))
        return lax.ppermute(x, ("dp", "row", "col"), pairs)

    def send_dp(x, chip_pairs, core_shift):
        pairs = [(z * cores + k, to * cores + (k + core_shift) % cores) for z, to in chip_pairs for k in range(cores)]
        return lax.ppermute(x, "dp", pairs)

    def matmul(x, y):
        return jnp.dot(x, y, preferred_element_type=jnp.float32)

    def shards(tokens, w_gate, w_up, w_down):
        r, c, d = lax.axis_index("row"), lax.axis_index("col"), lax.axis_index("dp")
        chip, core = d // cores, d % cores
        slab = w_gate.shape[0]
        hidden_width, width = w_down.shape
        half = width // 2
        at_b = core * half if turned else 0
        at_a = half - at_b

        def place(dr, dc):
            return (r + dr) % rows * cols + (c + dc) % cols

        def place_turned(a, b):
            return place(b + core * (a - b), a + core * (b - a)) if turned else place(b, a)

        def columns(x, at, size):
            return lax.dynamic_slice_in_dim(x, at, size, axis=1)

        early, late = [], []
        if turned:
            share = hidden_width // dp
            block = (rows - 1) * share
            piece = lax.dynamic_slice_in_dim(w_down, d * share, share, axis=0)
            along_col = [send(piece[:, :half], (0, -dc)) for dc in range(1, cols)]
            along_row = [send(piece[:, half:], (-dr, 0)) for dr in range(1, rows)]
            held = jnp.zeros((2 * block, half), jnp.bfloat16)
            for i in range(rows - 1):
                held = lax.dynamic_update_slice_in_dim(held, along_col[i], core * block + i * share, axis=0)
                held = lax.dynamic_update_slice_in_dim(held, along_row[i], (1 - core) * block + i * share, axis=0)

        feats = {s: columns(tokens, place(*s) * slab, slab) for s in shifts}
        got = {s: send(feats[s], s) for s in away}
        got[0, 0] = feats[0, 0]

        if line:
            two = send_dp(held, [(z, z ^ 2) for z in range(chips)], 0)
            one = send_dp(held, [(z, z ^ 1) for z in range(chips)], 0)
            middle = send_dp(held, [(1, 2), (2, 1)], 0)
            early += [(one, chip ^ 1), (two, chip ^ 2)]
        elif turned:
            for z in range(1, chips):
                turn = send_dp(held, [(i, (i + z) % chips) for i in range(chips)], 0)
                late.append((turn, (chip - z) % chips))

        def crossed(weight, col_first):
            first, second = (cols, rows) if col_first else (rows, cols)

            def shift(i, j):
                return (j, i) if col_first else (i, j)

            parts = {s: matmul(got[s], weight) for s in away}
            parts[0, 0] = matmul(got[0, 0], weight)
            sums = {j: parts[shift(0, j)] for j in range(second)}
            for j in reversed(range(second)):
                for i in range(1, first):
                    part = send(parts[shift(i, j)].astype(jnp.bfloat16), shift(-i, 0))
                    sums[j] = sums[j] + part.astype(jnp.float32)
            total = sums[0]
            passed = [sums[j].astype(jnp.bfloat16) for j in range(1, second)]
            for j in range(1, second):
                total = total + send(passed[j - 1], shift(0, -j)).astype(jnp.float32)
            return total, passed

        gate, gate_passed = crossed(w_gate, True)
        up, up_passed = crossed(w_up, False)
        hidden = (jax.nn.silu(gate) * up).astype(jnp.bfloat16)

        if turned:
            if line:
                relayed = send_dp(two, [(2, 3), (1, 0)], 0)
                late.append((jnp.where((chip == 0) | (chip == chips - 1), relayed, middle), chip ^ 3))
            far_b = {a: jnp.zeros((hidden_width, half), jnp.bfloat16) for a in range(1, rows)}
            far_a = {b: jnp.zeros((hidden_width, half), jnp.bfloat16) for b in range(1, rows)}

            def fill(pieces):
                for k in range(cores):
                    for moved, from_chip in pieces:
                        if k:
                            moved = send_dp(moved, [(z, z) for z in range(chips)], k)
                        at = (from_chip * cores + core + k * (1 - 2 * core)) * share
                        for i, far in enumerate([far_a, far_b] if k else [far_b, far_a]):
                            for j in range(1, rows):
                                lower = i * block + (j - 1) * share
                                far[j] = lax.dynamic_update_slice_in_dim(far[j], moved[lower : lower + share], at, axis=0)

            fill([(held, chip)])
            tied, _ = lax.optimization_barrier(([p for p, _ in early], gate_passed + up_passed))
            fill([(p, at) for p, (_, at) in zip(tied, early)])
        else:
            far_b = {a: send(w_down[:, :half], (0, -a)) for a in range(1, cols)}
            far_a = {b: send(w_down[:, half:], (-b, 0)) for b in range(1, rows)}

        near_b = {b: send_turned(hidden, (0, -b)) for b in far_a}
        near_a = {a: send_turned(hidden, (-a, 0)) for a in far_b}
        w_b, w_a = columns(w_down, at_b, half), columns(w_down, at_a, half)

        outs = []

        def give(x, weight, shift, slab_from, at):
            out = send_turned(matmul(x, weight).astype(jnp.bfloat16), shift)
            outs.append((out, place_turned(*slab_from) * width + at))

        for b, other in near_b.items():
            give(other, w_b, (0, b), (0, -b), at_b)
        for a, other in near_a.items():
            give(other, w_a, (a, 0), (-a, 0), at_a)
        if turned:
            tied, _ = lax.optimization_barrier(([p for p, _ in late], hidden))
            fill([(p, at) for p, (_, at) in zip(tied, late)])
        for b, other in near_b.items():
            for a in far_b:
                give(other, far_b[a], (0, b), (a, -b), at_b)
        for a, other in near_a.items():
            for b in far_a:
                give(other, far_a[b], (a, 0), (-a, b), at_a)

        def keep(weight):
            return matmul(hidden, weight).astype(jnp.bfloat16)

        landed = [(keep(w_down), place(0, 0) * width)]
        for a in far_b:
            landed.append((keep(far_b[a]), place_turned(a, 0) * width + at_b))
        for b in far_a:
            landed.append((keep(far_a[b]), place_turned(0, b) * width + at_a))
        mixed = jnp.zeros((tokens.shape[0], width * rows * cols), jnp.bfloat16)
        for block, at in landed + outs:
            mixed = lax.dynamic_update_slice_in_dim(mixed, block, at, axis=1)
        return mixed

    in_specs = (
        P(("dp", "row", "col"), None),
        P(("row", "col"), None),
        P(("row", "col"), None),
        P(None, ("row", "col")),
    )
    out_specs = P(("dp", "row", "col"), None)
    return jax.shard_map(shards, mesh=mesh, in_specs=in_specs, out_specs=out_specs, check_vma=False)
```

```python
import jax
import jax.numpy as jnp
from jax import lax
from jax.sharding import PartitionSpec as P


def solution(mesh):
    rows, cols, dp = mesh.shape["row"], mesh.shape["col"], mesh.shape["dp"]
    cores = 2 if dp % 2 == 0 else 1
    chips = dp // cores
    turned = cores == 2 and rows == cols
    line = turned and chips == 4
    shifts = [(dr, dc) for dr in range(rows) for dc in range(cols)]
    away = [s for s in shifts if s != (0, 0)]

    def send(x, shift):
        dr, dc = shift
        pairs = [
            (r * cols + c, (r + dr) % rows * cols + (c + dc) % cols) for r in range(rows) for c in range(cols)
        ]
        return lax.ppermute(x, ("row", "col"), pairs)

    def send_turned(x, shift):
        pairs = []
        for d in range(dp):
            dr, dc = shift if turned and d % cores else shift[::-1]
            for r in range(rows):
                for c in range(cols):
                    to = (d * rows + (r + dr) % rows) * cols + (c + dc) % cols
                    pairs.append(((d * rows + r) * cols + c, to))
        return lax.ppermute(x, ("dp", "row", "col"), pairs)

    def send_dp(x, chip_pairs, core_shift):
        pairs = [(z * cores + k, to * cores + (k + core_shift) % cores) for z, to in chip_pairs for k in range(cores)]
        return lax.ppermute(x, "dp", pairs)

    def matmul(x, y):
        return jnp.dot(x, y, preferred_element_type=jnp.float32)

    def shards(tokens, w_gate, w_up, w_down):
        r, c, d = lax.axis_index("row"), lax.axis_index("col"), lax.axis_index("dp")
        chip, core = d // cores, d % cores
        slab = w_gate.shape[0]
        hidden_width, width = w_down.shape
        half = width // 2
        at_b = core * half if turned else 0
        at_a = half - at_b

        def place(dr, dc):
            return (r + dr) % rows * cols + (c + dc) % cols

        def place_turned(a, b):
            return place(b + core * (a - b), a + core * (b - a)) if turned else place(b, a)

        def columns(x, at, size):
            return lax.dynamic_slice_in_dim(x, at, size, axis=1)

        early, late = [], []
        if turned:
            share = hidden_width // dp
            block = (rows - 1) * share
            piece = lax.dynamic_slice_in_dim(w_down, d * share, share, axis=0)
            along_col = [send(piece[:, :half], (0, -dc)) for dc in range(1, cols)]
            along_row = [send(piece[:, half:], (-dr, 0)) for dr in range(1, rows)]
            held = jnp.zeros((2 * block, half), jnp.bfloat16)
            for i in range(rows - 1):
                held = lax.dynamic_update_slice_in_dim(held, along_col[i], core * block + i * share, axis=0)
                held = lax.dynamic_update_slice_in_dim(held, along_row[i], (1 - core) * block + i * share, axis=0)

        feats = {s: columns(tokens, place(*s) * slab, slab) for s in shifts}
        got = {s: send(feats[s], s) for s in away}
        got[0, 0] = feats[0, 0]

        if line:
            two = send_dp(held, [(z, z ^ 2) for z in range(chips)], 0)
            one = send_dp(held, [(z, z ^ 1) for z in range(chips)], 0)
            middle = send_dp(held, [(1, 2), (2, 1)], 0)
            early += [(one, chip ^ 1), (two, chip ^ 2)]
        elif turned:
            for z in range(1, chips):
                turn = send_dp(held, [(i, (i + z) % chips) for i in range(chips)], 0)
                late.append((turn, (chip - z) % chips))

        def crossed(weight, col_first):
            first, second = (cols, rows) if col_first else (rows, cols)

            def shift(i, j):
                return (j, i) if col_first else (i, j)

            parts = {s: matmul(got[s], weight) for s in away}
            parts[0, 0] = matmul(got[0, 0], weight)
            sums = {j: parts[shift(0, j)] for j in range(second)}
            for j in reversed(range(second)):
                for i in range(1, first):
                    part = send(parts[shift(i, j)].astype(jnp.bfloat16), shift(-i, 0))
                    sums[j] = sums[j] + part.astype(jnp.float32)
            total = sums[0]
            passed = [sums[j].astype(jnp.bfloat16) for j in range(1, second)]
            for j in range(1, second):
                total = total + send(passed[j - 1], shift(0, -j)).astype(jnp.float32)
            return total, passed

        gate, gate_passed = crossed(w_gate, True)
        up, up_passed = crossed(w_up, False)
        hidden = (jax.nn.silu(gate) * up).astype(jnp.bfloat16)

        if turned:
            if line:
                relayed = send_dp(two, [(2, 3), (1, 0)], 0)
                late.append(((relayed, middle), chip ^ 3))
            far_b = {a: jnp.zeros((hidden_width, half), jnp.bfloat16) for a in range(1, rows)}
            far_a = {b: jnp.zeros((hidden_width, half), jnp.bfloat16) for b in range(1, rows)}

            def fill(pieces):
                for k in range(cores):
                    for moved, from_chip in pieces:
                        if k:
                            moved = send_dp(moved, [(z, z) for z in range(chips)], k)
                        at = (from_chip * cores + core + k * (1 - 2 * core)) * share
                        for i, far in enumerate([far_a, far_b] if k else [far_b, far_a]):
                            for j in range(1, rows):
                                lower = i * block + (j - 1) * share
                                far[j] = lax.dynamic_update_slice_in_dim(far[j], moved[lower : lower + share], at, axis=0)

            fill([(held, chip)])
            tied, _ = lax.optimization_barrier(([p for p, _ in early], gate_passed + up_passed))
            fill([(p, at) for p, (_, at) in zip(tied, early)])
        else:
            far_b = {a: send(w_down[:, :half], (0, -a)) for a in range(1, cols)}
            far_a = {b: send(w_down[:, half:], (-b, 0)) for b in range(1, rows)}

        near_b = {b: send_turned(hidden, (0, -b)) for b in far_a}
        near_a = {a: send_turned(hidden, (-a, 0)) for a in far_b}
        w_b, w_a = columns(w_down, at_b, half), columns(w_down, at_a, half)

        outs = []

        def give(x, weight, shift, slab_from, at):
            out = send_turned(matmul(x, weight).astype(jnp.bfloat16), shift)
            outs.append((out, place_turned(*slab_from) * width + at))

        for b, other in near_b.items():
            give(other, w_b, (0, b), (0, -b), at_b)
        for a, other in near_a.items():
            give(other, w_a, (a, 0), (-a, 0), at_a)
        if turned:
            tied, _ = lax.optimization_barrier(([p for p, _ in late], near_b))
            if line:
                tied = [jnp.where((chip == 0) | (chip == chips - 1), *tied[0])]
            fill([(p, at) for p, (_, at) in zip(tied, late)])
        for b, other in near_b.items():
            for a in far_b:
                give(other, far_b[a], (0, b), (a, -b), at_b)
        for a, other in near_a.items():
            for b in far_a:
                give(other, far_a[b], (a, 0), (-a, b), at_a)

        def keep(weight):
            return matmul(hidden, weight).astype(jnp.bfloat16)

        landed = [(keep(w_down), place(0, 0) * width)]
        for a in far_b:
            landed.append((keep(far_b[a]), place_turned(a, 0) * width + at_b))
        for b in far_a:
            landed.append((keep(far_a[b]), place_turned(0, b) * width + at_a))
        mixed = jnp.zeros((tokens.shape[0], width * rows * cols), jnp.bfloat16)
        for block, at in landed + outs:
            mixed = lax.dynamic_update_slice_in_dim(mixed, block, at, axis=1)
        return mixed

    in_specs = (
        P(("dp", "row", "col"), None),
        P(("row", "col"), None),
        P(("row", "col"), None),
        P(None, ("row", "col")),
    )
    out_specs = P(("dp", "row", "col"), None)
    return jax.shard_map(shards, mesh=mesh, in_specs=in_specs, out_specs=out_specs, check_vma=False)
```

```python
import jax
import jax.numpy as jnp
from jax import lax
from jax.sharding import PartitionSpec as P


def solution(mesh):
    rows, cols, dp = mesh.shape["row"], mesh.shape["col"], mesh.shape["dp"]
    cores = 2 if dp % 2 == 0 else 1
    chips = dp // cores
    turned = cores == 2 and rows == cols
    line = turned and chips == 4
    shifts = [(dr, dc) for dr in range(rows) for dc in range(cols)]
    away = [s for s in shifts if s != (0, 0)]

    def send(x, shift):
        dr, dc = shift
        pairs = [
            (r * cols + c, (r + dr) % rows * cols + (c + dc) % cols) for r in range(rows) for c in range(cols)
        ]
        return lax.ppermute(x, ("row", "col"), pairs)

    def send_turned(x, shift):
        pairs = []
        for d in range(dp):
            dr, dc = shift if turned and d % cores else shift[::-1]
            for r in range(rows):
                for c in range(cols):
                    to = (d * rows + (r + dr) % rows) * cols + (c + dc) % cols
                    pairs.append(((d * rows + r) * cols + c, to))
        return lax.ppermute(x, ("dp", "row", "col"), pairs)

    def send_dp(x, chip_pairs, core_shift):
        pairs = [(z * cores + k, to * cores + (k + core_shift) % cores) for z, to in chip_pairs for k in range(cores)]
        return lax.ppermute(x, "dp", pairs)

    def matmul(x, y):
        return jnp.dot(x, y, preferred_element_type=jnp.float32)

    def shards(tokens, w_gate, w_up, w_down):
        r, c, d = lax.axis_index("row"), lax.axis_index("col"), lax.axis_index("dp")
        chip, core = d // cores, d % cores
        slab = w_gate.shape[0]
        hidden_width, width = w_down.shape
        half = width // 2

        def place(dr, dc):
            return (r + dr) % rows * cols + (c + dc) % cols

        def columns(x, at, size):
            return lax.dynamic_slice_in_dim(x, at, size, axis=1)

        early, late = [], []
        if turned:
            share = hidden_width // chips
            piece = lax.dynamic_slice(w_down, (chip * share, core * half), (share, half))
            held = [send_turned(piece, (-a, 0)) for a in range(1, rows)]
            held = held[0] if len(held) == 1 else jnp.concatenate(held, axis=0)

        feats = {s: columns(tokens, place(*s) * slab, slab) for s in shifts}
        got = {s: send(feats[s], s) for s in away}
        got[0, 0] = feats[0, 0]

        if line:
            two = send_dp(held, [(z, z ^ 2) for z in range(chips)], 0)
            one = send_dp(held, [(z, z ^ 1) for z in range(chips)], 0)
            middle = send_dp(held, [(1, 2), (2, 1)], 0)
            early += [(one, chip ^ 1), (two, chip ^ 2)]
        elif turned:
            for z in range(1, chips):
                turn = send_dp(held, [(i, (i + z) % chips) for i in range(chips)], 0)
                late.append((turn, (chip - z) % chips))

        def crossed(weight, col_first):
            first, second = (cols, rows) if col_first else (rows, cols)

            def shift(i, j):
                return (j, i) if col_first else (i, j)

            parts = {s: matmul(got[s], weight) for s in away}
            parts[0, 0] = matmul(got[0, 0], weight)
            sums = {j: parts[shift(0, j)] for j in range(second)}
            for j in reversed(range(second)):
                for i in range(1, first):
                    part = send(parts[shift(i, j)].astype(jnp.bfloat16), shift(-i, 0))
                    sums[j] = sums[j] + part.astype(jnp.float32)
            total = sums[0]
            passed = [sums[j].astype(jnp.bfloat16) for j in range(1, second)]
            for j in range(1, second):
                total = total + send(passed[j - 1], shift(0, -j)).astype(jnp.float32)
            return total, passed

        gate, gate_passed = crossed(w_gate, True)
        up, up_passed = crossed(w_up, False)
        hidden = (jax.nn.silu(gate) * up).astype(jnp.bfloat16)

        if turned:
            if line:
                relayed = send_dp(two, [(2, 3), (1, 0)], 0)
                late.append(((relayed, middle), chip ^ 3))
            far = jnp.zeros((2 * (rows - 1) * hidden_width, half), jnp.bfloat16)

            def fill(far, pieces):
                for k in range(cores):
                    for moved, from_chip in pieces:
                        if k:
                            moved = send_dp(moved, [(z, z) for z in range(chips)], k)
                        group = core + k * (1 - 2 * core)
                        for i in range(rows - 1):
                            at = (group * (rows - 1) + i) * hidden_width + from_chip * share
                            far = lax.dynamic_update_slice_in_dim(far, moved[i * share : (i + 1) * share], at, axis=0)
                return far

            far = fill(far, [(held, chip)])
            tied, _ = lax.optimization_barrier(([p for p, _ in early], gate_passed + up_passed))
            far = fill(far, [(p, at) for p, (_, at) in zip(tied, early)])

        near = {(dr, 0): send(hidden, (-dr, 0)) for dr in range(1, rows)}
        near |= {(0, dc): send(hidden, (0, -dc)) for dc in range(1, cols)}

        outs = []

        def give(x, weight, shift, slab_from, at):
            out = send(matmul(x, weight).astype(jnp.bfloat16), shift)
            outs.append((out, place(*slab_from) * width + at))

        def keep(weight):
            return matmul(hidden, weight).astype(jnp.bfloat16)

        for (dr, dc), other in near.items():
            weight, at = (w_down[:, :half], 0) if dr else (w_down[:, half:], half)
            give(other, weight, (dr, dc), (-dr, -dc), at)
        if turned:
            tied, _ = lax.optimization_barrier(([p for p, _ in late], near))
            if line:
                tied = [jnp.where((chip == 0) | (chip == chips - 1), *tied[0])]
            far = fill(far, [(p, at) for p, (_, at) in zip(tied, late)])
            blocks = [far[i * hidden_width : (i + 1) * hidden_width] for i in range(2 * (rows - 1))]
            far_col = {dc: blocks[dc - 1] for dc in range(1, cols)}
            far_row = {dr: blocks[rows - 1 + dr - 1] for dr in range(1, rows)}
        else:
            far_col = {dc: send(w_down[:, :half], (0, -dc)) for dc in range(1, cols)}
            far_row = {dr: send(w_down[:, half:], (-dr, 0)) for dr in range(1, rows)}
        for (dr, dc), other in near.items():
            for i in far_col if dr else far_row:
                if dr:
                    give(other, far_col[i], (dr, 0), (-dr, i), 0)
                else:
                    give(other, far_row[i], (0, dc), (i, -dc), half)

        landed = [(keep(w_down), place(0, 0) * width)]
        for dc in far_col:
            landed.append((keep(far_col[dc]), place(0, dc) * width))
        for dr in far_row:
            landed.append((keep(far_row[dr]), place(dr, 0) * width + half))
        mixed = jnp.zeros((tokens.shape[0], width * rows * cols), jnp.bfloat16)
        for block, at in landed + outs:
            mixed = lax.dynamic_update_slice_in_dim(mixed, block, at, axis=1)
        return mixed

    in_specs = (
        P(("dp", "row", "col"), None),
        P(("row", "col"), None),
        P(("row", "col"), None),
        P(None, ("row", "col")),
    )
    out_specs = P(("dp", "row", "col"), None)
    return jax.shard_map(shards, mesh=mesh, in_specs=in_specs, out_specs=out_specs, check_vma=False)
```

```python
import jax
import jax.numpy as jnp
from jax import lax
from jax.sharding import PartitionSpec as P


def solution(mesh):
    rows, cols, dp = mesh.shape["row"], mesh.shape["col"], mesh.shape["dp"]
    cores = 2 if dp % 2 == 0 else 1
    chips = dp // cores
    shifts = [(dr, dc) for dr in range(rows) for dc in range(cols)]
    away = [s for s in shifts if s != (0, 0)]

    def send(x, shift):
        dr, dc = shift
        pairs = [
            (r * cols + c, (r + dr) % rows * cols + (c + dc) % cols) for r in range(rows) for c in range(cols)
        ]
        return lax.ppermute(x, ("row", "col"), pairs)

    def send_dp(x, chip_pairs, core_shift):
        pairs = [(z * cores + k, to * cores + (k + core_shift) % cores) for z, to in chip_pairs for k in range(cores)]
        return lax.ppermute(x, "dp", pairs)

    def swap(x, core_shift):
        return send_dp(x, [(z, z) for z in range(chips)], core_shift)

    def back(shift):
        return (-shift[0]) % rows, (-shift[1]) % cols

    def matmul(a, b):
        return jnp.dot(a, b, preferred_element_type=jnp.float32)

    def shards(tokens, w_gate, w_up, w_down):
        r, c, d = lax.axis_index("row"), lax.axis_index("col"), lax.axis_index("dp")
        chip, core = d // cores, d % cores
        slab = w_gate.shape[0]
        hidden_width, width = w_down.shape
        half = width // 2
        share = hidden_width // dp

        def place(shift):
            return (r + shift[0]) % rows * cols + (c + shift[1]) % cols

        piece = lax.dynamic_slice_in_dim(w_down, d * share, share, axis=0)
        sides = [(0, dc) for dc in range(1, cols)] + [(dr, 0) for dr in range(1, rows)]
        hopped = [send(piece[:, half:] if s[0] else piece[:, :half], back(s)) for s in sides]

        feats = {s: lax.dynamic_slice_in_dim(tokens, place(s) * slab, slab, axis=1) for s in shifts}
        got = {s: send(feats[s], s) for s in away}
        got[0, 0] = feats[0, 0]

        first_parts = [matmul(got[s], w).astype(jnp.bfloat16) for s in away if s[0] and s[1] for w in (w_gate, w_up)]
        hopped, _ = lax.optimization_barrier((hopped, first_parts))
        held = jnp.concatenate(hopped, axis=0)

        early, late = [], []
        if chips == 4:
            two = send_dp(held, [(z, z ^ 2) for z in range(chips)], 0)
            one = send_dp(held, [(z, z ^ 1) for z in range(chips)], 0)
            middle = send_dp(held, [(1, 2), (2, 1)], 0)
            early += [(one, chip ^ 1), (two, chip ^ 2)]
        else:
            for z in range(1, chips):
                turn = send_dp(held, [(i, (i + z) % chips) for i in range(chips)], 0)
                late.append((turn, (chip - z) % chips))

        def crossed(weight, col_first):
            first, second = (cols, rows) if col_first else (rows, cols)

            def shift(a, b):
                return (b, a) if col_first else (a, b)

            parts = {s: matmul(got[s], weight) for s in away}
            parts[0, 0] = matmul(got[0, 0], weight)
            sums = {b: parts[shift(0, b)] for b in range(second)}
            for b in reversed(range(second)):
                for a in range(1, first):
                    part = send(parts[shift(a, b)].astype(jnp.bfloat16), back(shift(a, 0)))
                    sums[b] = sums[b] + part.astype(jnp.float32)
            total = sums[0]
            passed = [sums[b].astype(jnp.bfloat16) for b in range(1, second)]
            for b in range(1, second):
                total = total + send(passed[b - 1], back(shift(0, b))).astype(jnp.float32)
            return total, passed

        gate, gate_passed = crossed(w_gate, True)
        up, up_passed = crossed(w_up, False)
        hidden = (jax.nn.silu(gate) * up).astype(jnp.bfloat16)

        if chips == 4:
            relayed = send_dp(two, [(2, 3), (1, 0)], 0)
            late.append((jnp.where((chip == 0) | (chip == chips - 1), relayed, middle), chip ^ 3))

        far = {s: jnp.zeros((hidden_width, half), jnp.bfloat16) for s in sides}

        def fill(pieces):
            for k in range(cores):
                for block, from_chip in pieces:
                    moved = swap(block, k) if k else block
                    at = (from_chip * cores + (core - k) % cores) * share
                    for i, s in enumerate(sides):
                        far[s] = lax.dynamic_update_slice_in_dim(far[s], moved[i * share : (i + 1) * share], at, axis=0)

        fill([(held, chip)])
        tied, _ = lax.optimization_barrier(([p for p, _ in early], gate_passed + up_passed))
        fill([(p, at) for p, (_, at) in zip(tied, early)])

        near = {s: send(hidden, back(s)) for s in reversed(sides)}
        landed = [(matmul(hidden, w_down).astype(jnp.bfloat16), place((0, 0)) * width)]
        outs = []
        for s, other in near.items():
            weight, at = (w_down[:, :half], 0) if s[1] == 0 else (w_down[:, half:], half)
            own_out = matmul(other, weight).astype(jnp.bfloat16)
            outs.append((send(own_out, s), place(back(s)) * width + at))

        tied, _ = lax.optimization_barrier(([p for p, _ in late], hidden))
        fill([(p, at) for p, (_, at) in zip(tied, late)])
        for s in sides:
            at = half if s[0] else 0
            landed.append((matmul(hidden, far[s]).astype(jnp.bfloat16), place(s) * width + at))
        for s, other in near.items():
            at = 0 if s[1] == 0 else half
            for t in sides:
                if (t[0] == 0) == (s[1] == 0):
                    far_out = send(matmul(other, far[t]).astype(jnp.bfloat16), s)
                    outs.append((far_out, place((t[0] - s[0], t[1] - s[1])) * width + at))
        landed += outs

        mixed = jnp.zeros((tokens.shape[0], width * rows * cols), jnp.bfloat16)
        for block, at in landed:
            mixed = lax.dynamic_update_slice_in_dim(mixed, block, at, axis=1)
        return mixed

    in_specs = (
        P(("dp", "row", "col"), None),
        P(("row", "col"), None),
        P(("row", "col"), None),
        P(None, ("row", "col")),
    )
    out_specs = P(("dp", "row", "col"), None)
    return jax.shard_map(shards, mesh=mesh, in_specs=in_specs, out_specs=out_specs, check_vma=False)
```

```python
import jax
import jax.numpy as jnp
from jax import lax
from jax.sharding import PartitionSpec as P


def solution(mesh):
    rows, cols, dp = mesh.shape["row"], mesh.shape["col"], mesh.shape["dp"]
    cores = 2 if dp % 2 == 0 else 1
    chips = dp // cores
    shifts = [(dr, dc) for dr in range(rows) for dc in range(cols)]
    away = [s for s in shifts if s != (0, 0)]

    def send(x, shift):
        dr, dc = shift
        pairs = [
            (r * cols + c, (r + dr) % rows * cols + (c + dc) % cols) for r in range(rows) for c in range(cols)
        ]
        return lax.ppermute(x, ("row", "col"), pairs)

    def send_dp(x, chip_pairs, core_shift):
        pairs = [(z * cores + k, to * cores + (k + core_shift) % cores) for z, to in chip_pairs for k in range(cores)]
        return lax.ppermute(x, "dp", pairs)

    def swap(x, core_shift):
        return send_dp(x, [(z, z) for z in range(chips)], core_shift)

    def back(shift):
        return (-shift[0]) % rows, (-shift[1]) % cols

    def matmul(a, b):
        return jnp.dot(a, b, preferred_element_type=jnp.float32)

    def shards(tokens, w_gate, w_up, w_down):
        r, c, d = lax.axis_index("row"), lax.axis_index("col"), lax.axis_index("dp")
        chip, core = d // cores, d % cores
        slab = w_gate.shape[0]
        hidden_width, width = w_down.shape
        half = width // 2
        share = hidden_width // dp

        def place(shift):
            return (r + shift[0]) % rows * cols + (c + shift[1]) % cols

        piece = lax.dynamic_slice_in_dim(w_down, d * share, share, axis=0)
        sides = [(0, dc) for dc in range(1, cols)] + [(dr, 0) for dr in range(1, rows)]
        held = jnp.concatenate([send(piece[:, half:] if s[0] else piece[:, :half], back(s)) for s in sides], axis=0)

        feats = {s: lax.dynamic_slice_in_dim(tokens, place(s) * slab, slab, axis=1) for s in shifts}
        got = {s: send(feats[s], s) for s in away}
        got[0, 0] = feats[0, 0]

        early, late = [], []
        if chips == 4:
            two_a = send_dp(held, [(0, 2), (3, 1)], 0)
            two_b = send_dp(held, [(1, 3), (2, 0)], 0)
            one = send_dp(held, [(z, z ^ 1) for z in range(chips)], 0)
            middle = send_dp(held, [(1, 2), (2, 1)], 0)
            relayed = send_dp(two_a, [(2, 3), (1, 0)], 0)
            outer = (chip == 0) | (chip == chips - 1)
            two = jnp.where(outer, two_b, two_a)
            early += [(one, chip ^ 1), (two, chip ^ 2)]
        else:
            for z in range(1, chips):
                turn = send_dp(held, [(i, (i + z) % chips) for i in range(chips)], 0)
                late.append((turn, (chip - z) % chips))

        def crossed(weight, col_first):
            first, second = (cols, rows) if col_first else (rows, cols)

            def shift(a, b):
                return (b, a) if col_first else (a, b)

            parts = {s: matmul(got[s], weight) for s in away}
            parts[0, 0] = matmul(got[0, 0], weight)
            sums = {b: parts[shift(0, b)] for b in range(second)}
            for b in reversed(range(second)):
                for a in range(1, first):
                    part = send(parts[shift(a, b)].astype(jnp.bfloat16), back(shift(a, 0)))
                    sums[b] = sums[b] + part.astype(jnp.float32)
            total = sums[0]
            passed = [sums[b].astype(jnp.bfloat16) for b in range(1, second)]
            for b in range(1, second):
                total = total + send(passed[b - 1], back(shift(0, b))).astype(jnp.float32)
            return total, passed

        gate, gate_passed = crossed(w_gate, True)
        up, up_passed = crossed(w_up, False)
        hidden = (jax.nn.silu(gate) * up).astype(jnp.bfloat16)

        if chips == 4:
            late.append((jnp.where(outer, relayed, middle), chip ^ 3))

        far = {s: jnp.zeros((hidden_width, half), jnp.bfloat16) for s in sides}

        def fill(pieces):
            for k in range(cores):
                for block, from_chip in pieces:
                    moved = swap(block, k) if k else block
                    at = (from_chip * cores + (core - k) % cores) * share
                    for i, s in enumerate(sides):
                        far[s] = lax.dynamic_update_slice_in_dim(far[s], moved[i * share : (i + 1) * share], at, axis=0)

        fill([(held, chip)])
        tied, _ = lax.optimization_barrier(([p for p, _ in early], gate_passed + up_passed))
        fill([(p, at) for p, (_, at) in zip(tied, early)])

        tied, _ = lax.optimization_barrier(([p for p, _ in late], hidden))
        fill([(p, at) for p, (_, at) in zip(tied, late)])
        near = {s: send(hidden, back(s)) for s in reversed(sides)}
        landed = [(matmul(hidden, w_down).astype(jnp.bfloat16), place((0, 0)) * width)]
        outs = []
        for s, other in near.items():
            weight, at = (w_down[:, :half], 0) if s[1] == 0 else (w_down[:, half:], half)
            own_out = matmul(other, weight).astype(jnp.bfloat16)
            outs.append((send(own_out, s), place(back(s)) * width + at))

        for s in sides:
            at = half if s[0] else 0
            landed.append((matmul(hidden, far[s]).astype(jnp.bfloat16), place(s) * width + at))
        for s, other in near.items():
            at = 0 if s[1] == 0 else half
            for t in sides:
                if (t[0] == 0) == (s[1] == 0):
                    far_out = send(matmul(other, far[t]).astype(jnp.bfloat16), s)
                    outs.append((far_out, place((t[0] - s[0], t[1] - s[1])) * width + at))
        landed += outs

        mixed = jnp.zeros((tokens.shape[0], width * rows * cols), jnp.bfloat16)
        for block, at in landed:
            mixed = lax.dynamic_update_slice_in_dim(mixed, block, at, axis=1)
        return mixed

    in_specs = (
        P(("dp", "row", "col"), None),
        P(("row", "col"), None),
        P(("row", "col"), None),
        P(None, ("row", "col")),
    )
    out_specs = P(("dp", "row", "col"), None)
    return jax.shard_map(shards, mesh=mesh, in_specs=in_specs, out_specs=out_specs, check_vma=False)
```

```python
import jax
import jax.numpy as jnp
from jax import lax
from jax.sharding import PartitionSpec as P


def solution(mesh):
    rows, cols, dp = mesh.shape["row"], mesh.shape["col"], mesh.shape["dp"]
    cores = 2 if dp % 2 == 0 else 1
    chips = dp // cores
    shifts = [(dr, dc) for dr in range(rows) for dc in range(cols)]
    away = [s for s in shifts if s != (0, 0)]

    def send(x, shift):
        dr, dc = shift
        pairs = [
            (r * cols + c, (r + dr) % rows * cols + (c + dc) % cols) for r in range(rows) for c in range(cols)
        ]
        return lax.ppermute(x, ("row", "col"), pairs)

    def send_dp(x, chip_pairs, core_shift):
        pairs = [(z * cores + k, to * cores + (k + core_shift) % cores) for z, to in chip_pairs for k in range(cores)]
        return lax.ppermute(x, "dp", pairs)

    def swap(x, core_shift):
        return send_dp(x, [(z, z) for z in range(chips)], core_shift)

    def back(shift):
        return (-shift[0]) % rows, (-shift[1]) % cols

    def matmul(a, b):
        return jnp.dot(a, b, preferred_element_type=jnp.float32)

    def shards(tokens, w_gate, w_up, w_down):
        r, c, d = lax.axis_index("row"), lax.axis_index("col"), lax.axis_index("dp")
        chip, core = d // cores, d % cores
        slab = w_gate.shape[0]
        hidden_width, width = w_down.shape
        cut = width * 9 // 16
        share = hidden_width // dp

        def place(shift):
            return (r + shift[0]) % rows * cols + (c + shift[1]) % cols

        piece = lax.dynamic_slice_in_dim(w_down, d * share, share, axis=0)
        sides = [(0, dc) for dc in range(1, cols)] + [(dr, 0) for dr in range(1, rows)]
        held = jnp.concatenate([send(piece[:, cut:] if s[0] else piece[:, :cut], back(s)) for s in sides], axis=1)
        ends = [(width - cut if s[0] else cut) for s in sides]
        ends = {s: (sum(ends[:i]), sum(ends[: i + 1])) for i, s in enumerate(sides)}

        feats = {s: lax.dynamic_slice_in_dim(tokens, place(s) * slab, slab, axis=1) for s in shifts}
        got = {s: send(feats[s], s) for s in away}
        got[0, 0] = feats[0, 0]

        early, late = [], []
        if chips == 4:
            two_a = send_dp(held, [(0, 2), (3, 1)], 0)
            two_b = send_dp(held, [(1, 3), (2, 0)], 0)
            one = send_dp(held, [(z, z ^ 1) for z in range(chips)], 0)
            middle = send_dp(held, [(1, 2), (2, 1)], 0)
            relayed = send_dp(two_a, [(2, 3), (1, 0)], 0)
            outer = (chip == 0) | (chip == chips - 1)
            two = jnp.where(outer, two_b, two_a)
            early += [(held, chip), (one, chip ^ 1), (two, chip ^ 2)]
        else:
            early.append((held, chip))
            for z in range(1, chips):
                turn = send_dp(held, [(i, (i + z) % chips) for i in range(chips)], 0)
                late.append((turn, (chip - z) % chips))

        def crossed(weight, col_first):
            first, second = (cols, rows) if col_first else (rows, cols)

            def shift(a, b):
                return (b, a) if col_first else (a, b)

            parts = {}
            for s in away:
                parts[s] = matmul(got[s], weight)
            parts[0, 0] = matmul(got[0, 0], weight)
            sums = {b: parts[shift(0, b)] for b in range(second)}
            for b in reversed(range(second)):
                for a in range(1, first):
                    part = send(parts[shift(a, b)].astype(jnp.bfloat16), back(shift(a, 0)))
                    sums[b] = sums[b] + part.astype(jnp.float32)
            total = sums[0]
            passed = [sums[b].astype(jnp.bfloat16) for b in range(1, second)]
            for b in range(1, second):
                total = total + send(passed[b - 1], back(shift(0, b))).astype(jnp.float32)
            return total, passed

        gate, gate_passed = crossed(w_gate, True)
        up, up_passed = crossed(w_up, False)
        hidden = (jax.nn.silu(gate) * up).astype(jnp.bfloat16)

        if chips == 4:
            late.append((jnp.where(outer, relayed, middle), chip ^ 3))

        far = {s: jnp.zeros((hidden_width, ends[s][1] - ends[s][0]), jnp.bfloat16) for s in sides}

        def fill(pieces):
            for k in range(cores):
                for block, from_chip in pieces:
                    moved = swap(block, k) if k else block
                    at = (from_chip * cores + (core - k) % cores) * share
                    for s in sides:
                        far[s] = lax.dynamic_update_slice_in_dim(far[s], moved[:, slice(*ends[s])], at, axis=0)

        tied, _ = lax.optimization_barrier(([p for p, _ in early], gate_passed + up_passed))
        fill([(p, at) for p, (_, at) in zip(tied, early)])

        tied, _ = lax.optimization_barrier(([p for p, _ in late], hidden))
        fill([(p, at) for p, (_, at) in zip(tied, late)])
        near = {s: send(hidden, back(s)) for s in reversed(sides)}
        landed = [(matmul(hidden, w_down).astype(jnp.bfloat16), place((0, 0)) * width)]
        outs = []
        for s, other in near.items():
            weight, at = (w_down[:, :cut], 0) if s[1] == 0 else (w_down[:, cut:], cut)
            own_out = matmul(other, weight).astype(jnp.bfloat16)
            outs.append((send(own_out, s), place(back(s)) * width + at))

        for s in sides:
            at = cut if s[0] else 0
            landed.append((matmul(hidden, far[s]).astype(jnp.bfloat16), place(s) * width + at))
        for s, other in near.items():
            at = 0 if s[1] == 0 else cut
            for t in sides:
                if (t[0] == 0) == (s[1] == 0):
                    far_out = send(matmul(other, far[t]).astype(jnp.bfloat16), s)
                    outs.append((far_out, place((t[0] - s[0], t[1] - s[1])) * width + at))
        landed += outs

        mixed = jnp.zeros((tokens.shape[0], width * rows * cols), jnp.bfloat16)
        for block, at in landed:
            mixed = lax.dynamic_update_slice_in_dim(mixed, block, at, axis=1)
        return mixed

    in_specs = (
        P(("dp", "row", "col"), None),
        P(("row", "col"), None),
        P(("row", "col"), None),
        P(None, ("row", "col")),
    )
    out_specs = P(("dp", "row", "col"), None)
    return jax.shard_map(shards, mesh=mesh, in_specs=in_specs, out_specs=out_specs, check_vma=False)
```

```python
import jax
import jax.numpy as jnp
from jax import lax
from jax.sharding import PartitionSpec as P


def solution(mesh):
    rows, cols, dp = mesh.shape["row"], mesh.shape["col"], mesh.shape["dp"]
    cores = 2 if dp % 2 == 0 else 1
    chips = dp // cores
    shifts = [(dr, dc) for dr in range(rows) for dc in range(cols)]
    away = [s for s in shifts if s != (0, 0)]

    def send(x, shift):
        dr, dc = shift
        pairs = [
            (r * cols + c, (r + dr) % rows * cols + (c + dc) % cols) for r in range(rows) for c in range(cols)
        ]
        return lax.ppermute(x, ("row", "col"), pairs)

    turned = cores == 2 and rows == cols
    line = turned and chips == 4

    def send_turned(x, step):
        pairs = []
        for d in range(dp):
            dr, dc = (step, 0) if d % cores else (0, step)
            for r in range(rows):
                for c in range(cols):
                    to = (d * rows + (r + dr) % rows) * cols + (c + dc) % cols
                    pairs.append(((d * rows + r) * cols + c, to))
        return lax.ppermute(x, ("dp", "row", "col"), pairs)

    def send_dp(x, chip_pairs, core_shift):
        pairs = [(z * cores + k, to * cores + (k + core_shift) % cores) for z, to in chip_pairs for k in range(cores)]
        return lax.ppermute(x, "dp", pairs)

    def swap(x, core_shift):
        return send_dp(x, [(z, z) for z in range(chips)], core_shift)

    def back(shift):
        return (-shift[0]) % rows, (-shift[1]) % cols

    def matmul(a, b):
        return jnp.dot(a, b, preferred_element_type=jnp.float32)

    def shards(tokens, w_gate, w_up, w_down):
        r, c, d = lax.axis_index("row"), lax.axis_index("col"), lax.axis_index("dp")
        chip, core = d // cores, d % cores
        slab = w_gate.shape[0]
        hidden_width, width = w_down.shape
        half = width // 2

        def place(shift):
            return (r + shift[0]) % rows * cols + (c + shift[1]) % cols

        sides = [(0, dc) for dc in range(1, cols)] + [(dr, 0) for dr in range(1, rows)]
        if turned:
            share = hidden_width // chips
            piece = lax.dynamic_slice(w_down, (chip * share, core * half), (share, half))
            parts_of = [piece[: share // 2], piece[share // 2 :]]
            held = jnp.concatenate([send_turned(x, -i) for i in range(1, rows) for x in parts_of], axis=0)

        feats = {s: lax.dynamic_slice_in_dim(tokens, place(s) * slab, slab, axis=1) for s in shifts}
        got = {s: send(feats[s], s) for s in away}
        got[0, 0] = feats[0, 0]

        early, late = [], []
        if line:
            two_a = send_dp(held, [(0, 2), (3, 1)], 0)
            two_b = send_dp(held, [(1, 3), (2, 0)], 0)
            one = send_dp(held, [(z, z ^ 1) for z in range(chips)], 0)
            middle = send_dp(held, [(1, 2), (2, 1)], 0)
            relayed = send_dp(two_a, [(2, 3), (1, 0)], 0)
            outer = (chip == 0) | (chip == chips - 1)
            two = jnp.where(outer, two_b, two_a)
            early += [(held, chip), (one, chip ^ 1), (two, chip ^ 2)]
        elif turned:
            early.append((held, chip))
            for z in range(1, chips):
                turn = send_dp(held, [(i, (i + z) % chips) for i in range(chips)], 0)
                late.append((turn, (chip - z) % chips))

        def crossed(weight, col_first):
            first, second = (cols, rows) if col_first else (rows, cols)

            def shift(a, b):
                return (b, a) if col_first else (a, b)

            parts = {}
            for s in away:
                parts[s] = matmul(got[s], weight)
            parts[0, 0] = matmul(got[0, 0], weight)
            sums = {b: parts[shift(0, b)] for b in range(second)}
            for b in reversed(range(second)):
                for a in range(1, first):
                    part = send(parts[shift(a, b)].astype(jnp.bfloat16), back(shift(a, 0)))
                    sums[b] = sums[b] + part.astype(jnp.float32)
            total = sums[0]
            passed = [sums[b].astype(jnp.bfloat16) for b in range(1, second)]
            for b in range(1, second):
                total = total + send(passed[b - 1], back(shift(0, b))).astype(jnp.float32)
            return total, passed

        gate, gate_passed = crossed(w_gate, True)
        up, up_passed = crossed(w_up, False)
        hidden = (jax.nn.silu(gate) * up).astype(jnp.bfloat16)

        if line:
            late.append((jnp.where(outer, relayed, middle), chip ^ 3))
        if turned:
            far = {s: jnp.zeros((hidden_width, half), jnp.bfloat16) for s in sides}

            def fill(pieces):
                for block, from_chip in pieces:
                    other = swap(block, 1)
                    for s in sides:
                        moved = jnp.where(core == (1 if s[0] else 0), block, other)
                        lower = (sum(s) - 1) * share
                        moved = moved[lower : lower + share]
                        far[s] = lax.dynamic_update_slice_in_dim(far[s], moved, from_chip * share, axis=0)

            tied, _ = lax.optimization_barrier(([p for p, _ in early], gate_passed + up_passed))
            fill([(p, at) for p, (_, at) in zip(tied, early)])
            tied, _ = lax.optimization_barrier(([p for p, _ in late], hidden))
            fill([(p, at) for p, (_, at) in zip(tied, late)])
        else:
            far = {s: send(w_down[:, half:] if s[0] else w_down[:, :half], back(s)) for s in sides}
        near = {s: send(hidden, back(s)) for s in reversed(sides)}
        landed = [(matmul(hidden, w_down).astype(jnp.bfloat16), place((0, 0)) * width)]
        outs = []
        for s, other in near.items():
            weight, at = (w_down[:, :half], 0) if s[1] == 0 else (w_down[:, half:], half)
            own_out = matmul(other, weight).astype(jnp.bfloat16)
            outs.append((send(own_out, s), place(back(s)) * width + at))

        for s in sides:
            at = half if s[0] else 0
            landed.append((matmul(hidden, far[s]).astype(jnp.bfloat16), place(s) * width + at))
        for s, other in near.items():
            at = 0 if s[1] == 0 else half
            for t in sides:
                if (t[0] == 0) == (s[1] == 0):
                    far_out = send(matmul(other, far[t]).astype(jnp.bfloat16), s)
                    outs.append((far_out, place((t[0] - s[0], t[1] - s[1])) * width + at))
        landed += outs

        mixed = jnp.zeros((tokens.shape[0], width * rows * cols), jnp.bfloat16)
        for block, at in landed:
            mixed = lax.dynamic_update_slice_in_dim(mixed, block, at, axis=1)
        return mixed

    in_specs = (
        P(("dp", "row", "col"), None),
        P(("row", "col"), None),
        P(("row", "col"), None),
        P(None, ("row", "col")),
    )
    out_specs = P(("dp", "row", "col"), None)
    return jax.shard_map(shards, mesh=mesh, in_specs=in_specs, out_specs=out_specs, check_vma=False)
```

```python
import jax
import jax.numpy as jnp
from jax import lax
from jax.sharding import PartitionSpec as P


def solution(mesh):
    rows, cols, dp = mesh.shape["row"], mesh.shape["col"], mesh.shape["dp"]
    cores = 2 if dp % 2 == 0 else 1
    chips = dp // cores
    shifts = [(dr, dc) for dr in range(rows) for dc in range(cols)]
    away = [s for s in shifts if s != (0, 0)]

    def send(x, shift):
        dr, dc = shift
        pairs = [
            (r * cols + c, (r + dr) % rows * cols + (c + dc) % cols) for r in range(rows) for c in range(cols)
        ]
        return lax.ppermute(x, ("row", "col"), pairs)

    turned = cores == 2 and rows == cols

    def send_turned(x, step, along_row):
        pairs = []
        for d in range(dp):
            dr, dc = (step, 0) if along_row != bool(d % cores) else (0, step)
            for r in range(rows):
                for c in range(cols):
                    to = (d * rows + (r + dr) % rows) * cols + (c + dc) % cols
                    pairs.append(((d * rows + r) * cols + c, to))
        return lax.ppermute(x, ("dp", "row", "col"), pairs)

    def send_dp(x, chip_pairs, core_shift):
        pairs = [(z * cores + k, to * cores + (k + core_shift) % cores) for z, to in chip_pairs for k in range(cores)]
        return lax.ppermute(x, "dp", pairs)

    def swap(x, core_shift):
        return send_dp(x, [(z, z) for z in range(chips)], core_shift)

    def back(shift):
        return (-shift[0]) % rows, (-shift[1]) % cols

    def matmul(a, b):
        return jnp.dot(a, b, preferred_element_type=jnp.float32)

    def shards(tokens, w_gate, w_up, w_down):
        r, c, d = lax.axis_index("row"), lax.axis_index("col"), lax.axis_index("dp")
        chip, core = d // cores, d % cores
        slab = w_gate.shape[0]
        hidden_width, width = w_down.shape
        half = width // 2
        share = hidden_width // dp

        def place(shift):
            return (r + shift[0]) % rows * cols + (c + shift[1]) % cols

        piece = lax.dynamic_slice_in_dim(w_down, d * share, share, axis=0)
        sides = [(0, dc) for dc in range(1, cols)] + [(dr, 0) for dr in range(1, rows)]
        if turned:
            held = jnp.zeros((len(sides) * share, half), jnp.bfloat16)
            for turn in range(2):
                kind = turn + core * (1 - 2 * turn)
                block = lax.dynamic_slice_in_dim(piece, kind * half, half, axis=1)
                for i in range(1, rows):
                    got_block = send_turned(block, -i, bool(turn))
                    at = (kind * (rows - 1) + i - 1) * share
                    held = lax.dynamic_update_slice_in_dim(held, got_block, at, axis=0)
        else:
            held = jnp.concatenate([send(piece[:, half:] if s[0] else piece[:, :half], back(s)) for s in sides], axis=0)

        feats = {s: lax.dynamic_slice_in_dim(tokens, place(s) * slab, slab, axis=1) for s in shifts}
        got = {s: send(feats[s], s) for s in away}
        got[0, 0] = feats[0, 0]

        early, late = [], []
        if chips == 4:
            two_a = send_dp(held, [(0, 2), (3, 1)], 0)
            two_b = send_dp(held, [(1, 3), (2, 0)], 0)
            one = send_dp(held, [(z, z ^ 1) for z in range(chips)], 0)
            middle = send_dp(held, [(1, 2), (2, 1)], 0)
            relayed = send_dp(two_a, [(2, 3), (1, 0)], 0)
            outer = (chip == 0) | (chip == chips - 1)
            two = jnp.where(outer, two_b, two_a)
            early += [(held, chip), (one, chip ^ 1), (two, chip ^ 2)]
        else:
            early.append((held, chip))
            for z in range(1, chips):
                turn = send_dp(held, [(i, (i + z) % chips) for i in range(chips)], 0)
                late.append((turn, (chip - z) % chips))

        def crossed(weight, col_first):
            first, second = (cols, rows) if col_first else (rows, cols)

            def shift(a, b):
                return (b, a) if col_first else (a, b)

            parts = {}
            for s in away:
                parts[s] = matmul(got[s], weight)
            parts[0, 0] = matmul(got[0, 0], weight)
            sums = {b: parts[shift(0, b)] for b in range(second)}
            for b in reversed(range(second)):
                for a in range(1, first):
                    part = send(parts[shift(a, b)].astype(jnp.bfloat16), back(shift(a, 0)))
                    sums[b] = sums[b] + part.astype(jnp.float32)
            total = sums[0]
            passed = [sums[b].astype(jnp.bfloat16) for b in range(1, second)]
            for b in range(1, second):
                total = total + send(passed[b - 1], back(shift(0, b))).astype(jnp.float32)
            return total, passed

        gate, gate_passed = crossed(w_gate, True)
        up, up_passed = crossed(w_up, False)
        hidden = (jax.nn.silu(gate) * up).astype(jnp.bfloat16)

        if chips == 4:
            late.append((jnp.where(outer, relayed, middle), chip ^ 3))

        far = {s: jnp.zeros((hidden_width, half), jnp.bfloat16) for s in sides}

        def fill(pieces):
            for k in range(cores):
                for block, from_chip in pieces:
                    moved = swap(block, k) if k else block
                    at = (from_chip * cores + (core - k) % cores) * share
                    for i, s in enumerate(sides):
                        far[s] = lax.dynamic_update_slice_in_dim(far[s], moved[i * share : (i + 1) * share], at, axis=0)

        tied, _ = lax.optimization_barrier(([p for p, _ in early], gate_passed + up_passed))
        fill([(p, at) for p, (_, at) in zip(tied, early)])

        tied, _ = lax.optimization_barrier(([p for p, _ in late], hidden))
        fill([(p, at) for p, (_, at) in zip(tied, late)])
        near = {s: send(hidden, back(s)) for s in sides}
        landed = [(matmul(hidden, w_down).astype(jnp.bfloat16), place((0, 0)) * width)]
        outs = []
        for s, other in near.items():
            weight, at = (w_down[:, :half], 0) if s[1] == 0 else (w_down[:, half:], half)
            own_out = matmul(other, weight).astype(jnp.bfloat16)
            outs.append((send(own_out, s), place(back(s)) * width + at))

        for s in sides:
            at = half if s[0] else 0
            landed.append((matmul(hidden, far[s]).astype(jnp.bfloat16), place(s) * width + at))
        for s, other in near.items():
            at = 0 if s[1] == 0 else half
            for t in sides:
                if (t[0] == 0) == (s[1] == 0):
                    far_out = send(matmul(other, far[t]).astype(jnp.bfloat16), s)
                    outs.append((far_out, place((t[0] - s[0], t[1] - s[1])) * width + at))
        landed += outs

        mixed = jnp.zeros((tokens.shape[0], width * rows * cols), jnp.bfloat16)
        for block, at in landed:
            mixed = lax.dynamic_update_slice_in_dim(mixed, block, at, axis=1)
        return mixed

    in_specs = (
        P(("dp", "row", "col"), None),
        P(("row", "col"), None),
        P(("row", "col"), None),
        P(None, ("row", "col")),
    )
    out_specs = P(("dp", "row", "col"), None)
    return jax.shard_map(shards, mesh=mesh, in_specs=in_specs, out_specs=out_specs, check_vma=False)
```

```python
import jax
import jax.numpy as jnp
from jax import lax
from jax.sharding import PartitionSpec as P


def solution(mesh):
    rows, cols, dp = mesh.shape["row"], mesh.shape["col"], mesh.shape["dp"]
    cores = 2 if dp % 2 == 0 else 1
    chips = dp // cores
    shifts = [(dr, dc) for dr in range(rows) for dc in range(cols)]
    away = [s for s in shifts if s != (0, 0)]

    def send(x, shift):
        dr, dc = shift
        pairs = [
            (r * cols + c, (r + dr) % rows * cols + (c + dc) % cols) for r in range(rows) for c in range(cols)
        ]
        return lax.ppermute(x, ("row", "col"), pairs)

    turned = cores == 2 and rows == cols

    def send_turned(x, step, along_row):
        pairs = []
        for d in range(dp):
            dr, dc = (step, 0) if along_row != bool(d % cores) else (0, step)
            for r in range(rows):
                for c in range(cols):
                    to = (d * rows + (r + dr) % rows) * cols + (c + dc) % cols
                    pairs.append(((d * rows + r) * cols + c, to))
        return lax.ppermute(x, ("dp", "row", "col"), pairs)

    def send_dp(x, chip_pairs, core_shift):
        pairs = [(z * cores + k, to * cores + (k + core_shift) % cores) for z, to in chip_pairs for k in range(cores)]
        return lax.ppermute(x, "dp", pairs)

    def swap(x, core_shift):
        return send_dp(x, [(z, z) for z in range(chips)], core_shift)

    def back(shift):
        return (-shift[0]) % rows, (-shift[1]) % cols

    def matmul(a, b):
        return jnp.dot(a, b, preferred_element_type=jnp.float32)

    def shards(tokens, w_gate, w_up, w_down):
        r, c, d = lax.axis_index("row"), lax.axis_index("col"), lax.axis_index("dp")
        chip, core = d // cores, d % cores
        slab = w_gate.shape[0]
        hidden_width, width = w_down.shape
        half = width // 2
        share = hidden_width // dp

        def place(shift):
            return (r + shift[0]) % rows * cols + (c + shift[1]) % cols

        piece = lax.dynamic_slice_in_dim(w_down, d * share, share, axis=0)
        sides = [(0, dc) for dc in range(1, cols)] + [(dr, 0) for dr in range(1, rows)]
        if turned:
            held = jnp.zeros((len(sides) * share, half), jnp.bfloat16)
            for turn in range(2):
                kind = turn + core * (1 - 2 * turn)
                block = lax.dynamic_slice_in_dim(piece, kind * half, half, axis=1)
                for i in range(1, rows):
                    got_block = send_turned(block, -i, bool(turn))
                    at = (kind * (rows - 1) + i - 1) * share
                    held = lax.dynamic_update_slice_in_dim(held, got_block, at, axis=0)
        else:
            held = jnp.concatenate([send(piece[:, half:] if s[0] else piece[:, :half], back(s)) for s in sides], axis=0)

        def features(x, s):
            return lax.dynamic_slice_in_dim(x, place(s) * slab, slab, axis=1)

        feats = {s: features(tokens, s) for s in shifts if not (s[0] and s[1])}
        again, _ = lax.optimization_barrier((tokens, [feats[s] for s in feats if s != (0, 0)]))
        feats |= {s: features(again, s) for s in shifts if s[0] and s[1]}
        got = {s: send(feats[s], s) for s in away}
        got[0, 0] = feats[0, 0]

        early, late = [], []
        if chips == 4:
            two_a = send_dp(held, [(0, 2), (3, 1)], 0)
            two_b = send_dp(held, [(1, 3), (2, 0)], 0)
            one = send_dp(held, [(z, z ^ 1) for z in range(chips)], 0)
            middle = send_dp(held, [(1, 2), (2, 1)], 0)
            relayed = send_dp(two_a, [(2, 3), (1, 0)], 0)
            outer = (chip == 0) | (chip == chips - 1)
            two = jnp.where(outer, two_b, two_a)
            early += [(held, chip), (one, chip ^ 1), (two, chip ^ 2)]
        else:
            early.append((held, chip))
            for z in range(1, chips):
                turn = send_dp(held, [(i, (i + z) % chips) for i in range(chips)], 0)
                late.append((turn, (chip - z) % chips))

        def crossed(weight, col_first):
            first, second = (cols, rows) if col_first else (rows, cols)

            def shift(a, b):
                return (b, a) if col_first else (a, b)

            parts = {}
            for s in away:
                parts[s] = matmul(got[s], weight)
            parts[0, 0] = matmul(got[0, 0], weight)
            sums = {b: parts[shift(0, b)] for b in range(second)}
            for b in reversed(range(second)):
                for a in range(1, first):
                    part = send(parts[shift(a, b)].astype(jnp.bfloat16), back(shift(a, 0)))
                    sums[b] = sums[b] + part.astype(jnp.float32)
            total = sums[0]
            passed = [sums[b].astype(jnp.bfloat16) for b in range(1, second)]
            for b in range(1, second):
                total = total + send(passed[b - 1], back(shift(0, b))).astype(jnp.float32)
            return total, passed

        gate, gate_passed = crossed(w_gate, True)
        up, up_passed = crossed(w_up, False)
        hidden = (jax.nn.silu(gate) * up).astype(jnp.bfloat16)

        if chips == 4:
            late.append((jnp.where(outer, relayed, middle), chip ^ 3))

        far = {s: jnp.zeros((hidden_width, half), jnp.bfloat16) for s in sides}

        def fill(pieces):
            for k in range(cores):
                for block, from_chip in pieces:
                    moved = swap(block, k) if k else block
                    at = (from_chip * cores + (core - k) % cores) * share
                    for i, s in enumerate(sides):
                        far[s] = lax.dynamic_update_slice_in_dim(far[s], moved[i * share : (i + 1) * share], at, axis=0)

        tied, _ = lax.optimization_barrier(([p for p, _ in early], gate_passed + up_passed))
        fill([(p, at) for p, (_, at) in zip(tied, early)])

        tied, _ = lax.optimization_barrier(([p for p, _ in late], hidden))
        fill([(p, at) for p, (_, at) in zip(tied, late)])
        near = {s: send(hidden, back(s)) for s in sides}
        landed = [(matmul(hidden, w_down).astype(jnp.bfloat16), place((0, 0)) * width)]
        outs = []
        for s, other in near.items():
            weight, at = (w_down[:, :half], 0) if s[1] == 0 else (w_down[:, half:], half)
            own_out = matmul(other, weight).astype(jnp.bfloat16)
            outs.append((send(own_out, s), place(back(s)) * width + at))

        for s in sides:
            at = half if s[0] else 0
            landed.append((matmul(hidden, far[s]).astype(jnp.bfloat16), place(s) * width + at))
        for s, other in near.items():
            at = 0 if s[1] == 0 else half
            for t in sides:
                if (t[0] == 0) == (s[1] == 0):
                    far_out = send(matmul(other, far[t]).astype(jnp.bfloat16), s)
                    outs.append((far_out, place((t[0] - s[0], t[1] - s[1])) * width + at))
        landed += outs

        mixed = jnp.zeros((tokens.shape[0], width * rows * cols), jnp.bfloat16)
        for block, at in landed:
            mixed = lax.dynamic_update_slice_in_dim(mixed, block, at, axis=1)
        return mixed

    in_specs = (
        P(("dp", "row", "col"), None),
        P(("row", "col"), None),
        P(("row", "col"), None),
        P(None, ("row", "col")),
    )
    out_specs = P(("dp", "row", "col"), None)
    return jax.shard_map(shards, mesh=mesh, in_specs=in_specs, out_specs=out_specs, check_vma=False)
```

```python
import jax
import jax.numpy as jnp
from jax import lax
from jax.sharding import PartitionSpec as P


def solution(mesh):
    rows, cols, dp = mesh.shape["row"], mesh.shape["col"], mesh.shape["dp"]
    cores = 2 if dp % 2 == 0 else 1
    chips = dp // cores
    shifts = [(dr, dc) for dr in range(rows) for dc in range(cols)]
    away = [s for s in shifts if s != (0, 0)]

    def send(x, shift):
        dr, dc = shift
        pairs = [
            (r * cols + c, (r + dr) % rows * cols + (c + dc) % cols) for r in range(rows) for c in range(cols)
        ]
        return lax.ppermute(x, ("row", "col"), pairs)

    def send_dp(x, chip_pairs, core_shift):
        pairs = [(z * cores + k, to * cores + (k + core_shift) % cores) for z, to in chip_pairs for k in range(cores)]
        return lax.ppermute(x, "dp", pairs)

    def swap(x, core_shift):
        return send_dp(x, [(z, z) for z in range(chips)], core_shift)

    def back(shift):
        return (-shift[0]) % rows, (-shift[1]) % cols

    def matmul(a, b):
        return jnp.dot(a, b, preferred_element_type=jnp.float32)

    def shards(tokens, w_gate, w_up, w_down):
        r, c, d = lax.axis_index("row"), lax.axis_index("col"), lax.axis_index("dp")
        chip, core = d // cores, d % cores
        slab = w_gate.shape[0]
        hidden_width, width = w_down.shape
        half = width // 2
        share = hidden_width // dp

        def place(shift):
            return (r + shift[0]) % rows * cols + (c + shift[1]) % cols

        piece = lax.dynamic_slice_in_dim(w_down, d * share, share, axis=0)
        sides = [(0, dc) for dc in range(1, cols)] + [(dr, 0) for dr in range(1, rows)]
        held = jnp.concatenate([send(piece[:, half:] if s[0] else piece[:, :half], back(s)) for s in sides], axis=0)

        feats = {s: lax.dynamic_slice_in_dim(tokens, place(s) * slab, slab, axis=1) for s in shifts}
        got = {s: send(feats[s], s) for s in away}
        got[0, 0] = feats[0, 0]

        early, late = [], []
        if chips == 4:
            two_a = send_dp(held, [(0, 2), (3, 1)], 0)
            two_b = send_dp(held, [(1, 3), (2, 0)], 0)
            one = send_dp(held, [(z, z ^ 1) for z in range(chips)], 0)
            middle = send_dp(held, [(1, 2), (2, 1)], 0)
            relayed = send_dp(two_a, [(2, 3), (1, 0)], 0)
            outer = (chip == 0) | (chip == chips - 1)
            two = jnp.where(outer, two_b, two_a)
            early += [(held, chip), (one, chip ^ 1), (two, chip ^ 2)]
        else:
            early.append((held, chip))
            for z in range(1, chips):
                turn = send_dp(held, [(i, (i + z) % chips) for i in range(chips)], 0)
                late.append((turn, (chip - z) % chips))

        def crossed(weight, col_first):
            first, second = (cols, rows) if col_first else (rows, cols)

            def shift(a, b):
                return (b, a) if col_first else (a, b)

            parts = {}
            for s in away:
                parts[s] = matmul(got[s], weight)
            parts[0, 0] = matmul(got[0, 0], weight)
            sums = {b: parts[shift(0, b)] for b in range(second)}
            for b in reversed(range(second)):
                for a in range(1, first):
                    part = send(parts[shift(a, b)].astype(jnp.bfloat16), back(shift(a, 0)))
                    sums[b] = sums[b] + part.astype(jnp.float32)
            total = sums[0]
            passed = [sums[b].astype(jnp.bfloat16) for b in range(1, second)]
            for b in range(1, second):
                total = total + send(passed[b - 1], back(shift(0, b))).astype(jnp.float32)
            return total, passed

        gate, gate_passed = crossed(w_gate, True)
        up, up_passed = crossed(w_up, False)
        hidden = (jax.nn.silu(gate) * up).astype(jnp.bfloat16)

        if chips == 4:
            late.append((jnp.where(outer, relayed, middle), chip ^ 3))

        far = {s: jnp.zeros((hidden_width, half), jnp.bfloat16) for s in sides}

        def fill(pieces):
            for k in range(cores):
                for block, from_chip in pieces:
                    moved = swap(block, k) if k else block
                    at = (from_chip * cores + (core - k) % cores) * share
                    for i, s in enumerate(sides):
                        far[s] = lax.dynamic_update_slice_in_dim(far[s], moved[i * share : (i + 1) * share], at, axis=0)

        tied, _ = lax.optimization_barrier(([p for p, _ in early], gate_passed + up_passed))
        fill([(p, at) for p, (_, at) in zip(tied, early)])

        tied, _ = lax.optimization_barrier(([p for p, _ in late], hidden))
        fill([(p, at) for p, (_, at) in zip(tied, late)])
        near = {s: send(hidden, back(s)) for s in reversed(sides)}
        landed = [(matmul(hidden, w_down).astype(jnp.bfloat16), place((0, 0)) * width)]
        outs = []
        for s, other in near.items():
            weight, at = (w_down[:, :half], 0) if s[1] == 0 else (w_down[:, half:], half)
            own_out = matmul(other, weight).astype(jnp.bfloat16)
            outs.append((send(own_out, s), place(back(s)) * width + at))

        for s in sides:
            at = half if s[0] else 0
            landed.append((matmul(hidden, far[s]).astype(jnp.bfloat16), place(s) * width + at))
        for s, other in near.items():
            at = 0 if s[1] == 0 else half
            for t in sides:
                if (t[0] == 0) == (s[1] == 0):
                    far_out = send(matmul(other, far[t]).astype(jnp.bfloat16), s)
                    outs.append((far_out, place((t[0] - s[0], t[1] - s[1])) * width + at))
        landed += outs

        mixed = jnp.zeros((tokens.shape[0], width * rows * cols), jnp.bfloat16)
        for block, at in landed:
            mixed = lax.dynamic_update_slice_in_dim(mixed, block, at, axis=1)
        return mixed

    in_specs = (
        P(("dp", "row", "col"), None),
        P(("row", "col"), None),
        P(("row", "col"), None),
        P(None, ("row", "col")),
    )
    out_specs = P(("dp", "row", "col"), None)
    return jax.shard_map(shards, mesh=mesh, in_specs=in_specs, out_specs=out_specs, check_vma=False)
```
